32 devices in a mesh: pairs: 1 (over z), cols: 4 (over y), rows: 8 (over x, core).
Axes of the slice: x: 4, y: 4, z: 1, core: 2. Of those that a mesh axis runs over, the one named last changes fastest.
The devices are a block of a 4x4x8 slice.
Arguments:
- C1: float32 [8192, 8192], P(('pairs', 'rows'), 'cols')
- C2: float32 [1024, 1024], P(('pairs', 'rows'), 'cols')
- T0: float32 [8192, 1024], P(('pairs', 'rows'), 'cols')
- p: float32 [8192], P(('pairs', 'rows'))
- q: float32 [1024], P(('pairs', 'cols'))
- eps: float32 [8], P('pairs')
Outputs:
- output 1: float32 [8192, 1024], P(('pairs', 'rows'), 'cols')
- output 2: float32 [1], P('pairs')
All inputs are finite; a program needn't handle non-finite values.
Results may differ from the reference program's by a relative error of at most 0.001.
Values are sent between devices in bfloat16 or wider.
A program may use at most 768 MiB of HBM per device.

```python
import jax
import jax.numpy as jnp
from jax import lax

N = 8192
M = 1024
DX = 3
DY = 3
OUTER = 8
SWEEPS = 10
CLUSTERS = 8
PROBE = 256


def cloud_dists(key, count, dim):
    subkeys = jax.random.split(key, 4)
    labels = jax.random.randint(subkeys[0], (count,), 0, CLUSTERS)
    centers = jax.random.normal(subkeys[1], (CLUSTERS, dim), jnp.float32)
    widths = jax.random.uniform(subkeys[2], (CLUSTERS, 1), jnp.float32, 0.2, 0.6)
    points = centers[labels] + widths[labels] * jax.random.normal(subkeys[3], (count, dim), jnp.float32)
    sq_norm = jnp.sum(points * points, axis=1)
    dists = jnp.maximum(sq_norm[:, None] + sq_norm[None, :] - 2.0 * jnp.dot(points, points.T), 0.0)
    dists = 0.5 * (dists + dists.T) * (1.0 - jnp.eye(count, dtype=jnp.float32))
    return points, dists / jnp.max(dists)


def point_features(key, points):
    projection = jax.random.normal(key, (points.shape[1], 4), jnp.float32)
    embedded = jnp.dot(points, projection)
    embedded = embedded - jnp.mean(embedded, axis=0)
    return embedded / jnp.std(embedded, axis=0)


def eps_schedule(key, C1, C2, T0, p, q):
    probe_rows = min(N, PROBE)
    c1_probe = C1[:probe_rows]
    lead_mat = jnp.dot(c1_probe, T0)
    cost_mat = jnp.dot(c1_probe * c1_probe, p)[:, None] + jnp.dot(C2 * C2, q)[None, :] - 2.0 * jnp.dot(lead_mat, C2)
    spread = jnp.mean(jnp.max(cost_mat, axis=1) - jnp.min(cost_mat, axis=1))
    ratios = jax.random.uniform(key, (OUTER,), jnp.float32, 6.0, 14.0)
    return spread / ratios


def setup_inputs(seed: int = 0, part: int = 0) -> dict:
    key = jax.random.fold_in(jax.random.key(seed), part)
    subkeys = jax.random.split(key, 7)
    points_x, C1 = cloud_dists(subkeys[0], N, DX)
    points_y, C2 = cloud_dists(subkeys[1], M, DY)
    p_raw = jax.random.uniform(subkeys[2], (N,), jnp.float32, 0.25, 1.75)
    q_raw = jax.random.uniform(subkeys[3], (M,), jnp.float32, 0.25, 1.75)
    p = p_raw / jnp.sum(p_raw)
    q = q_raw / jnp.sum(q_raw)
    feat_x = point_features(subkeys[4], points_x)
    feat_y = point_features(subkeys[5], points_y)
    tilt_map = 1.0 + 0.8 * jnp.tanh(0.5 * jnp.dot(feat_x, feat_y.T))
    T0 = p[:, None] * q[None, :] * tilt_map
    T0 = T0 / jnp.sum(T0)
    eps = eps_schedule(subkeys[6], C1, C2, T0, p, q)
    return {"C1": C1, "C2": C2, "T0": T0, "p": p, "q": q, "eps": eps}


def reference(C1, C2, T0, p, q, eps):
    c1_half = C1.astype(jnp.bfloat16)
    c2_half = C2.astype(jnp.bfloat16)
    const_c = jnp.dot(C1 * C1, p)[:, None] + jnp.dot(C2 * C2, q)[None, :]

    def cost_of(plan_mat):
        lead_mat = jnp.dot(c1_half, plan_mat.astype(jnp.bfloat16), preferred_element_type=jnp.float32)
        cross_mat = jnp.dot(lead_mat.astype(jnp.bfloat16), c2_half, preferred_element_type=jnp.float32)
        return const_c - 2.0 * cross_mat

    def outer_step(plan_mat, eps_step):
        cost_mat = cost_of(plan_mat)
        kernel = jnp.exp(-(cost_mat - jnp.min(cost_mat, axis=1, keepdims=True)) / eps_step)

        def sweep(sweep_idx, scales):
            row_scale = p / jnp.sum(kernel * scales[1][None, :], axis=1)
            col_scale = q / jnp.sum(kernel * row_scale[:, None], axis=0)
            return row_scale, col_scale

        row_scale, col_scale = lax.fori_loop(0, SWEEPS, sweep, (jnp.ones_like(p), jnp.ones_like(q)))
        return row_scale[:, None] * kernel * col_scale[None, :], eps_step

    plan_mat = lax.scan(outer_step, T0, eps)[0]
    loss_val = jnp.sum(cost_of(plan_mat) * plan_mat)
    return plan_mat, loss_val.reshape(1)
```

```python
import functools

import jax
import jax.numpy as jnp
from jax import lax
from jax.experimental import pallas as pl
from jax.experimental.pallas import tpu as pltpu
from jax.sharding import PartitionSpec as P

SWEEPS = 10
MESH = pl.DeviceIdType.MESH
BLK = 128


def gw_kernel(n_rows, n_cols, n_steps, eps_ref, c1_ref, c2_ref, t0_ref, p_ref, q_ref, a_ref, b_ref,
              t_ref, loss_ref, tp, ap, lead, cross, kern, u_ref, red,
              t_send, t_recv, a_send, a_recv, s_send, s_recv):
    me_r = lax.axis_index("rows")
    me_c = lax.axis_index("cols")
    chip, core = me_r // 2, me_r % 2
    n_chips = n_rows // 2
    height = t0_ref.shape[0]
    width = t0_ref.shape[1]
    half = height // 2

    def row_id(chip_off, core_sel):
        return ((chip + chip_off + n_chips) % n_chips) * 2 + core_sel

    sib = row_id(0, 1 - core)
    right, left = row_id(1, core), row_id(-1, core)
    up, down = (me_c + 1) % n_cols, (me_c + n_cols - 1) % n_cols

    barrier = pltpu.get_barrier_semaphore()
    for d in range(1, n_rows):
        pl.semaphore_signal(barrier, inc=1, device_id={"rows": (me_r + d) % n_rows}, device_id_type=MESH)
    for other in (up, down):
        pl.semaphore_signal(barrier, inc=1, device_id={"cols": other}, device_id_type=MESH)
    pl.semaphore_wait(barrier, n_rows + 1)

    def t_copy(slot, part, target, send_idx):
        ref = tp.at[slot, pl.ds(part * half, half)]
        return pltpu.make_async_remote_copy(src_ref=ref, dst_ref=ref, send_sem=t_send.at[send_idx],
                                            recv_sem=t_recv.at[slot, part], device_id={"rows": target}, device_id_type=MESH)

    def a_copy(par, slot, part, target, send_idx):
        ref = ap.at[par, slot, pl.ds(part * half, half)]
        return pltpu.make_async_remote_copy(src_ref=ref, dst_ref=ref, send_sem=a_send.at[send_idx],
                                            recv_sem=a_recv.at[par, slot, part], device_id={"cols": target}, device_id_type=MESH)

    def lead_add(slot, first):
        cols = pl.ds(pl.multiple_of(slot * height, height), height)
        prod = jnp.dot(c1_ref[:, cols], tp[slot], preferred_element_type=jnp.float32)
        if first:
            lead[...] = prod
        else:
            lead[...] += prod

    def cross_add(par, slot, first):
        rows = pl.ds(pl.multiple_of(slot * width, width), width)
        prod = jnp.dot(ap[par, slot], c2_ref[rows, :], preferred_element_type=jnp.float32)
        if first:
            cross[...] = prod
        else:
            cross[...] += prod

    def cost(step):
        sent = []

        def send(slot, part, target):
            copy = t_copy(slot, part, target, len(sent))
            copy.start()
            sent.append(copy)

        def recv(slot, part):
            t_copy(slot, part, sib, 0).wait_recv()

        for part in (0, 1):
            send(me_r, part, right)
            send(me_r, 1 - part, left)
        for part in (0, 1):
            send(me_r, part, sib)
        lead_add(me_r, True)
        recv(sib, 0)
        recv(sib, 1)
        lead_add(sib, False)
        recv(left, 0)
        send(left, 0, right)
        send(left, 0, sib)
        recv(right, 1)
        send(right, 1, left)
        send(right, 1, sib)
        recv(left, 1)
        send(left, 1, sib)
        recv(right, 0)
        send(right, 0, sib)
        lead_add(left, False)
        lead_add(right, False)
        for off in (-1, 1):
            slot = row_id(off, 1 - core)
            recv(slot, 0)
            recv(slot, 1)
            lead_add(slot, False)
        far = row_id(2, core)
        for part in (0, 1):
            recv(far, part)
            send(far, part, sib)
        lead_add(far, False)
        far_sib = row_id(2, 1 - core)
        recv(far_sib, 0)
        recv(far_sib, 1)
        lead_add(far_sib, False)
        for copy in sent:
            copy.wait_send()

        par = step % 2
        ap[par, me_c] = lead[...].astype(jnp.bfloat16)
        sent_a = []

        def send_a(slot, part, target):
            copy = a_copy(par, slot, part, target, len(sent_a))
            copy.start()
            sent_a.append(copy)

        def recv_a(slot, part):
            a_copy(par, slot, part, up, 0).wait_recv()

        for part in (0, 1):
            send_a(me_c, part, up)
            send_a(me_c, 1 - part, down)
        cross_add(par, me_c, True)
        recv_a(down, 0)
        send_a(down, 0, up)
        recv_a(up, 1)
        send_a(up, 1, down)
        recv_a(down, 1)
        cross_add(par, down, False)
        recv_a(up, 0)
        cross_add(par, up, False)
        opp = (me_c + 2) % n_cols
        recv_a(opp, 0)
        recv_a(opp, 1)
        cross_add(par, opp, False)
        for copy in sent_a:
            copy.wait_send()

    def group_sum(par, value):
        red[par, me_r] = value
        copies = []
        for d in range(1, n_rows):
            other = (me_r + d) % n_rows
            copy = pltpu.make_async_remote_copy(src_ref=red.at[par, me_r], dst_ref=red.at[par, me_r],
                                                send_sem=s_send.at[par, d - 1], recv_sem=s_recv.at[par, me_r],
                                                device_id={"rows": other}, device_id_type=MESH)
            copy.start()
            copies.append(copy)
        for d in range(1, n_rows):
            other = (me_r + d) % n_rows
            pltpu.make_async_remote_copy(src_ref=red.at[par, other], dst_ref=red.at[par, other],
                                         send_sem=s_send.at[par, d - 1], recv_sem=s_recv.at[par, other],
                                         device_id={"rows": other}, device_id_type=MESH).wait_recv()
        total = red[par, 0]
        for d in range(1, n_rows):
            total = total + red[par, d]
        for copy in copies:
            copy.wait_send()
        return total

    n_blk = height // BLK

    def fold(block):
        return jnp.sum(block.reshape(BLK // 8, 8, block.shape[1]), axis=0)

    def make_kernel(step):
        inv_eps = 1.0 / jnp.full((1, 1), eps_ref[step], jnp.float32)
        for k in range(n_blk):
            rows = pl.ds(k * BLK, BLK)
            block = (a_ref[rows, :] + b_ref[...]) - 2.0 * cross[rows, :]
            low = jnp.min(block, axis=1, keepdims=True)
            kern[rows, :] = jnp.exp((low - block) * inv_eps)

    def sweep(par, v):
        acc = jnp.zeros((8, v.shape[1]), jnp.float32)
        for k in range(n_blk):
            rows = pl.ds(k * BLK, BLK)
            u = p_ref[rows, :] / jnp.sum(kern[rows, :] * v, axis=1, keepdims=True)
            u_ref[rows, :] = u
            acc = acc + fold(kern[rows, :] * u)
        total = group_sum(par, jnp.sum(acc, axis=0, keepdims=True))
        return q_ref[...] / total

    my_cols = pl.ds(pl.multiple_of(me_c * width, width), width)
    v_ref = loss_ref

    def outer(step, carry):
        cost(step)

        @pl.when(step < n_steps)
        def _():
            make_kernel(step)

            def two_sweeps(i, v):
                return sweep(1, sweep(0, v))

            v = lax.fori_loop(0, SWEEPS // 2, two_sweeps, jnp.ones_like(q_ref))
            v_ref[...] = v
            for k in range(n_blk):
                rows = pl.ds(k * BLK, BLK)
                plan = u_ref[rows, :] * kern[rows, my_cols] * v_ref[:, my_cols]
                t_ref[rows, :] = plan
                tp[me_r, rows, :] = plan.astype(jnp.bfloat16)

        return carry

    tp[me_r] = t0_ref[...].astype(jnp.bfloat16)
    lax.fori_loop(0, n_steps + 1, outer, 0)

    v = v_ref[...]
    acc = jnp.zeros((8, v.shape[1]), jnp.float32)
    for k in range(n_blk):
        rows = pl.ds(k * BLK, BLK)
        block = (a_ref[rows, :] + b_ref[...]) - 2.0 * cross[rows, :]
        acc = acc + fold(block * (u_ref[rows, :] * kern[rows, :] * v))
    total = group_sum(0, jnp.sum(acc, axis=0, keepdims=True))
    loss_ref[...] = jnp.broadcast_to(jnp.sum(total, axis=1, keepdims=True), loss_ref.shape)


def solution(mesh):
    grid_spec = P(("pairs", "rows"), "cols")
    n_rows, n_cols = mesh.shape["rows"], mesh.shape["cols"]

    def local_fn(c1_blk, c2_blk, t0_blk, p_blk, q_blk, eps_blk):
        col_pos = lax.axis_index("cols")
        row_pos = lax.axis_index("rows")
        c1_width = c1_blk.shape[1]
        c2_height = c2_blk.shape[0]
        height, width = t0_blk.shape
        full = width * n_cols
        p_full = lax.all_gather(p_blk, "rows", tiled=True)
        q_full = lax.all_gather(q_blk, "cols", tiled=True)
        p_piece = lax.dynamic_slice_in_dim(p_full, col_pos * c1_width, c1_width)
        q_piece = lax.dynamic_slice_in_dim(q_full, row_pos * c2_height, c2_height)
        row_term = lax.psum(jnp.sum(c1_blk * c1_blk * p_piece[None, :], axis=1), "cols")
        col_blk = lax.psum(jnp.sum(c2_blk * c2_blk * q_piece[:, None], axis=0), "rows")
        col_term = lax.all_gather(col_blk, "cols", tiled=True)
        c1_panel = lax.all_gather(c1_blk.astype(jnp.bfloat16), "cols", axis=1, tiled=True)
        c2_panel = lax.all_gather(c2_blk.astype(jnp.bfloat16), "rows", axis=0, tiled=True)
        c2_full = lax.all_gather(c2_panel, "cols", axis=1, tiled=True)
        n_steps = eps_blk.shape[0]
        vmem = pl.BlockSpec(memory_space=pltpu.VMEM)
        f32, b16, dma = jnp.float32, jnp.bfloat16, pltpu.SemaphoreType.DMA
        plan, loss = pl.pallas_call(
            functools.partial(gw_kernel, n_rows, n_cols, n_steps),
            out_shape=(jax.ShapeDtypeStruct((height, width), f32), jax.ShapeDtypeStruct((1, full), f32)),
            in_specs=[pl.BlockSpec(memory_space=pltpu.SMEM)] + [vmem] * 7,
            out_specs=(vmem, vmem),
            scratch_shapes=[
                pltpu.VMEM((n_rows, height, width), b16),
                pltpu.VMEM((2, n_cols, height, width), b16),
                pltpu.VMEM((height, width), f32),
                pltpu.VMEM((height, full), f32),
                pltpu.VMEM((height, full), f32),
                pltpu.VMEM((height, 1), f32),
                pltpu.VMEM((2, n_rows, 1, full), f32),
                dma((14,)), dma((n_rows, 2)), dma((6,)), dma((2, n_cols, 2)),
                dma((2, n_rows - 1)), dma((2, n_rows)),
            ],
            compiler_params=pltpu.CompilerParams(collective_id=0, has_side_effects=True, vmem_limit_bytes=60 * 2**20),
        )(eps_blk, c1_panel, c2_full, t0_blk, p_blk[:, None], q_full[None, :], row_term[:, None], col_term[None, :])
        return plan, loss[0, :1]

    return jax.shard_map(local_fn, mesh=mesh, in_specs=(grid_spec, grid_spec, grid_spec, P(("pairs", "rows")), P(("pairs", "cols")), P("pairs")), out_specs=(grid_spec, P("pairs")), check_vma=False)
```

```python
import functools

import jax
import jax.numpy as jnp
from jax import lax
from jax.experimental import pallas as pl
from jax.experimental.pallas import tpu as pltpu
from jax.sharding import PartitionSpec as P

SWEEPS = 10
MESH = pl.DeviceIdType.MESH
BLK = 128
LANES = 128
PIECE = 256


def gw_kernel(n_rows, n_cols, n_steps, eps_ref, c1_ref, c2_ref, t0_ref, p_ref, q_ref,
              t_ref, loss_ref, c1s, tp, ap, lead, cross, kern, u_ref, red,
              stage, a_acc, a_col, p_col, b_row, q_row, c2f, c2s, p_all, q_all, b_all, b_red, a_red,
              t_send, t_recv, a_send, a_recv, s_send, s_recv, c_send, c_recv, x_send, x_recv, ld_sem):
    me_r = lax.axis_index("rows")
    me_c = lax.axis_index("cols")
    chip, core = me_r // 2, me_r % 2
    n_chips = n_rows // 2
    height, width = t0_ref.shape
    half = height // 2
    n_chunk = width // LANES
    n_piece = c1_ref.shape[1] // PIECE
    per_slot = height // PIECE
    n_blk = height // BLK

    def row_id(chip_off, core_sel):
        return ((chip + chip_off + n_chips) % n_chips) * 2 + core_sel

    sib = row_id(0, 1 - core)
    right, left, far = row_id(1, core), row_id(-1, core), row_id(2, core)
    up, down, opp = (me_c + 1) % n_cols, (me_c + n_cols - 1) % n_cols, (me_c + 2) % n_cols

    barrier = pltpu.get_barrier_semaphore()
    for d in range(1, n_rows):
        pl.semaphore_signal(barrier, inc=1, device_id={"rows": (me_r + d) % n_rows}, device_id_type=MESH)
    for d in range(1, n_cols):
        pl.semaphore_signal(barrier, inc=1, device_id={"cols": (me_c + d) % n_cols}, device_id_type=MESH)
    pl.semaphore_wait(barrier, n_rows + n_cols - 2)

    def share(idx, axis, ref_of):
        me, n = (me_r, n_rows) if axis == "rows" else (me_c, n_cols)

        def copy(slot, d):
            return pltpu.make_async_remote_copy(src_ref=ref_of(slot), dst_ref=ref_of(slot), send_sem=x_send.at[idx, d],
                                                recv_sem=x_recv.at[idx, slot], device_id={axis: (me + d) % n}, device_id_type=MESH)

        for d in range(1, n):
            copy(me, d).start()

        def finish():
            for d in range(1, n):
                copy((me + d) % n, d).wait_recv()
            for d in range(1, n):
                copy(me, d).wait_send()

        return finish

    def group_sum(par, value):
        red[par, me_r] = value
        copies = []
        for d in range(1, n_rows):
            other = (me_r + d) % n_rows
            copy = pltpu.make_async_remote_copy(src_ref=red.at[par, me_r], dst_ref=red.at[par, me_r],
                                                send_sem=s_send.at[par, d - 1], recv_sem=s_recv.at[par, me_r],
                                                device_id={"rows": other}, device_id_type=MESH)
            copy.start()
            copies.append(copy)
        for d in range(1, n_rows):
            other = (me_r + d) % n_rows
            pltpu.make_async_remote_copy(src_ref=red.at[par, other], dst_ref=red.at[par, other],
                                         send_sem=s_send.at[par, d - 1], recv_sem=s_recv.at[par, other],
                                         device_id={"rows": other}, device_id_type=MESH).wait_recv()
        total = red[par, 0]
        for d in range(1, n_rows):
            total = total + red[par, d]
        for copy in copies:
            copy.wait_send()
        return total

    def t_copy(slot, chunk, part, target, send_idx):
        ref = tp.at[slot, chunk, pl.ds(part * half, half)]
        return pltpu.make_async_remote_copy(src_ref=ref, dst_ref=ref, send_sem=t_send.at[chunk, send_idx],
                                            recv_sem=t_recv.at[slot, chunk, part], device_id={"rows": target}, device_id_type=MESH)

    t_sent = []

    def t_push(slot, chunk, part, target, send_idx):
        copy = t_copy(slot, chunk, part, target, send_idx)
        copy.start()
        t_sent.append(copy)

    def t_take(slot, chunk, part):
        t_copy(slot, chunk, part, sib, 0).wait_recv()

    def t_start(chunk):
        for part in (0, 1):
            t_push(me_r, chunk, part, right, part)
            t_push(me_r, chunk, 1 - part, left, 2 + part)
        for part in (0, 1):
            t_push(me_r, chunk, part, sib, 4 + part)

    def t_near(chunk):
        t_take(left, chunk, 0)
        t_push(left, chunk, 0, right, 6)
        t_take(right, chunk, 1)
        t_push(right, chunk, 1, left, 7)
        t_push(left, chunk, 0, sib, 8)
        t_push(right, chunk, 1, sib, 9)

    def t_rest(chunk):
        t_take(left, chunk, 1)
        t_push(left, chunk, 1, sib, 10)
        t_take(right, chunk, 0)
        t_push(right, chunk, 0, sib, 11)

    def t_far(chunk):
        for part in (0, 1):
            t_take(far, chunk, part)
            t_push(far, chunk, part, sib, 12 + part)

    def t_sib(chunk, chip_off):
        slot = row_id(chip_off, 1 - core)
        t_take(slot, chunk, 0)
        t_take(slot, chunk, 1)
        return slot

    def t_done():
        for copy in t_sent:
            copy.wait_send()
        t_sent.clear()

    def a_copy(par, slot, chunk, part, target, send_idx):
        ref = ap.at[par, slot, chunk, pl.ds(part * half, half)]
        return pltpu.make_async_remote_copy(src_ref=ref, dst_ref=ref, send_sem=a_send.at[chunk, send_idx],
                                            recv_sem=a_recv.at[par, slot, chunk, part], device_id={"cols": target}, device_id_type=MESH)

    a_sent = []

    def a_push(par, slot, chunk, part, target, send_idx):
        copy = a_copy(par, slot, chunk, part, target, send_idx)
        copy.start()
        a_sent.append(copy)

    def a_take(par, slot, chunk, part):
        a_copy(par, slot, chunk, part, up, 0).wait_recv()

    def a_start(par, chunk):
        ap[par, me_c, chunk] = lead[chunk].astype(jnp.bfloat16)
        for part in (0, 1):
            a_push(par, me_c, chunk, part, up, part)
            a_push(par, me_c, chunk, 1 - part, down, 2 + part)

    def a_near(par, chunk):
        a_take(par, down, chunk, 0)
        a_push(par, down, chunk, 0, up, 4)
        a_take(par, up, chunk, 1)
        a_push(par, up, chunk, 1, down, 5)

    def a_rest(par, chunk):
        a_take(par, down, chunk, 1)
        a_take(par, up, chunk, 0)

    def a_far(par, chunk):
        a_take(par, opp, chunk, 0)
        a_take(par, opp, chunk, 1)

    def a_done():
        for copy in a_sent:
            copy.wait_send()
        a_sent.clear()

    def c1_slot(slot):
        return jnp.concatenate([c1s[slot * per_slot + j] for j in range(per_slot)], axis=1)

    def lead_add(slot, chunk, first=False):
        prod = jnp.dot(c1_slot(slot), tp[slot, chunk], preferred_element_type=jnp.float32)
        lead[chunk] = prod if first else lead[chunk] + prod

    def lead_both(slot):
        plan = jnp.concatenate([tp[slot, k] for k in range(n_chunk)], axis=1)
        prod = jnp.dot(c1_slot(slot), plan, preferred_element_type=jnp.float32)
        for k in range(n_chunk):
            lead[k] = lead[k] + prod[:, k * LANES:(k + 1) * LANES]

    def cross_add(par, slot, first=False):
        rows = pl.ds(pl.multiple_of(slot * width, width), width)
        block = jnp.concatenate([ap[par, slot, k] for k in range(n_chunk)], axis=1)
        prod = jnp.dot(block, c2s[rows, :], preferred_element_type=jnp.float32)
        cross[...] = prod if first else cross[...] + prod

    def cross_all(par):
        cross_add(par, me_c, True)

    def piece_load(i):
        cols = pl.ds(pl.multiple_of(i * PIECE, PIECE), PIECE)
        return pltpu.make_async_copy(c1_ref.at[:, cols], stage.at[i % 2], ld_sem.at[i % 2])

    def piece_copy(piece, target, send_idx):
        return pltpu.make_async_remote_copy(src_ref=c1s.at[piece], dst_ref=c1s.at[piece], send_sem=c_send.at[send_idx],
                                            recv_sem=c_recv.at[piece], device_id={"cols": target}, device_id_type=MESH)

    def prologue():
        piece_load(0).start()
        p_all[me_r] = p_ref[...]
        p_fin = share(0, "rows", lambda s: p_all.at[s])
        q_all[me_c] = q_ref[...]
        q_fin = share(1, "cols", lambda s: q_all.at[s])
        c2f[me_r, me_c] = c2_ref[...].astype(jnp.bfloat16)
        c2y_fin = share(2, "cols", lambda s: c2f.at[me_r, s])
        for k in range(n_chunk):
            tp[me_r, k] = t0_ref[:, k * LANES:(k + 1) * LANES].astype(jnp.bfloat16)
        for k in range(n_chunk):
            t_start(k)
        a_acc[...] = jnp.zeros_like(a_acc)
        p_fin()

        def own_piece(i, carry):
            piece_load(i).wait()

            @pl.when(i + 1 < n_piece)
            def _():
                piece_load(i + 1).start()

            block = stage[i % 2]
            piece = me_c * n_piece + i
            c1s[piece] = block.astype(jnp.bfloat16)
            piece_copy(piece, up, i).start()
            piece_copy(piece, down, n_piece + i).start()
            where = piece * PIECE
            p_row = p_all[where // height, :, pl.ds(pl.multiple_of(where % height, PIECE), PIECE)]
            sq = block * block * p_row
            acc = a_acc[...]
            for k in range(PIECE // LANES):
                acc = acc + sq[:, k * LANES:(k + 1) * LANES]
            a_acc[...] = acc
            return carry

        lax.fori_loop(0, n_piece, own_piece, 0)
        q_fin()
        q_row[...] = jnp.concatenate([q_all[k] for k in range(n_cols)], axis=1)
        a_red[me_c] = jnp.sum(a_acc[...].T, axis=0, keepdims=True)
        a_fin = share(3, "cols", lambda s: a_red.at[s])
        low = me_r * c2_ref.shape[0]
        q_piece = q_all[low // width, :, pl.ds(pl.multiple_of(low % width, LANES), LANES)]
        q_col = jnp.broadcast_to(q_piece, (LANES, LANES)).T
        sq = c2_ref[...] * c2_ref[...]
        b_red[me_r] = jnp.sum(sq * q_col[:, :1], axis=0, keepdims=True)
        b_fin = share(4, "rows", lambda s: b_red.at[s])
        p_col[...] = jnp.broadcast_to(p_ref[...], (LANES, height)).T[:, :1]
        c2y_fin()
        c2x_fin = share(5, "rows", lambda s: c2f.at[s])
        for k in range(n_chunk):
            t_near(k)
        for k in range(n_chunk):
            t_rest(k)
        b_fin()
        total = b_red[0]
        for s in range(1, n_rows):
            total = total + b_red[s]
        b_all[me_c] = total
        ball_fin = share(6, "cols", lambda s: b_all.at[s])
        for k in range(n_chunk):
            t_far(k)
        for k in range(n_chunk):
            for off in (0, -1, 1, 2):
                t_sib(k, off)
        t_done()
        lead[...] = jnp.zeros_like(lead)

        def group(which):
            def body(j, carry):
                lead_both(which * (n_piece // per_slot) + j)
                return carry

            lax.fori_loop(0, n_piece // per_slot, body, 0)

        group(me_c)
        hop = n_piece // 2
        for i in range(n_piece):
            piece_copy(down * n_piece + i, up, 0).wait_recv()
            if i < hop:
                piece_copy(down * n_piece + i, up, 2 * n_piece + i).start()
            piece_copy(up * n_piece + i, up, 0).wait_recv()
            if i >= hop:
                piece_copy(up * n_piece + i, down, 2 * n_piece + i).start()
        group(down)
        group(up)
        a_fin()
        total = a_red[0]
        for s in range(1, n_cols):
            total = total + a_red[s]
        a_col[...] = jnp.broadcast_to(total, (LANES, height)).T[:, :1]
        ball_fin()
        b_row[...] = jnp.concatenate([b_all[k] for k in range(n_cols)], axis=1)
        c2x_fin()
        depth = c2_ref.shape[0]
        for r in range(n_rows):
            for c in range(n_cols):
                c2s[r * depth:(r + 1) * depth, c * width:(c + 1) * width] = c2f[r, c]
        for i in range(n_piece):
            piece_copy(opp * n_piece + i, up, 0).wait_recv()
        group(opp)
        for i in range(n_piece):
            piece_copy(me_c * n_piece + i, up, i).wait_send()
            piece_copy(me_c * n_piece + i, down, n_piece + i).wait_send()
            if i < hop:
                piece_copy(down * n_piece + i, up, 2 * n_piece + i).wait_send()
            else:
                piece_copy(up * n_piece + i, down, 2 * n_piece + i).wait_send()

        for k in range(n_chunk):
            a_start(0, k)
        cross_add(0, me_c, True)
        for k in range(n_chunk):
            a_near(0, k)
        for k in range(n_chunk):
            a_rest(0, k)
        cross_add(0, down)
        cross_add(0, up)
        for k in range(n_chunk):
            a_far(0, k)
        cross_add(0, opp)
        a_done()

    def cost(par):
        def early(chunk):
            lead_add(me_r, chunk, True)
            lead_add(t_sib(chunk, 0), chunk)

        def middle(chunk):
            t_rest(chunk)
            lead_add(left, chunk)
            lead_add(right, chunk)
            lead_add(t_sib(chunk, -1), chunk)
            lead_add(t_sib(chunk, 1), chunk)

        def late(chunk):
            t_far(chunk)
            lead_add(far, chunk)
            lead_add(t_sib(chunk, 2), chunk)
            a_start(par, chunk)

        t_start(0)
        early(0)
        t_near(0)
        t_start(1)
        middle(0)
        early(1)
        late(0)
        t_near(1)
        middle(1)
        a_near(par, 0)
        late(1)
        a_rest(par, 0)
        cross_add(par, me_c, True)
        a_near(par, 1)
        a_rest(par, 1)
        cross_add(par, down)
        cross_add(par, up)
        a_far(par, 0)
        a_far(par, 1)
        cross_add(par, opp)
        t_done()
        a_done()

    def fold(block):
        return jnp.sum(block.reshape(BLK // 8, 8, block.shape[1]), axis=0)

    def make_kernel(step):
        inv_eps = 1.0 / jnp.full((1, 1), eps_ref[step], jnp.float32)
        for k in range(n_blk):
            rows = pl.ds(k * BLK, BLK)
            block = (a_col[rows, :] + b_row[...]) - 2.0 * cross[rows, :]
            low = jnp.min(block, axis=1, keepdims=True)
            kern[rows, :] = jnp.exp((low - block) * inv_eps)

    def sweep(par, v):
        acc = jnp.zeros((8, v.shape[1]), jnp.float32)
        for k in range(n_blk):
            rows = pl.ds(k * BLK, BLK)
            u = p_col[rows, :] / jnp.sum(kern[rows, :] * v, axis=1, keepdims=True)
            u_ref[rows, :] = u
            acc = acc + fold(kern[rows, :] * u)
        total = group_sum(par, jnp.sum(acc, axis=0, keepdims=True))
        return q_row[...] / total

    v_ref = loss_ref

    def outer(step, carry):
        make_kernel(step)

        def two_sweeps(i, v):
            return sweep(1, sweep(0, v))

        v_ref[...] = lax.fori_loop(0, SWEEPS // 2, two_sweeps, jnp.ones_like(q_row))
        for c in range(n_chunk):
            cols = pl.ds(pl.multiple_of(me_c * width + c * LANES, LANES), LANES)
            for k in range(n_blk):
                rows = pl.ds(k * BLK, BLK)
                plan = u_ref[rows, :] * kern[rows, cols] * v_ref[:, cols]
                t_ref[rows, c * LANES:(c + 1) * LANES] = plan
                tp[me_r, c, rows, :] = plan.astype(jnp.bfloat16)
        cost((step + 1) % 2)
        return carry

    prologue()
    lax.fori_loop(0, n_steps, outer, 0)

    v = v_ref[...]
    acc = jnp.zeros((8, v.shape[1]), jnp.float32)
    for k in range(n_blk):
        rows = pl.ds(k * BLK, BLK)
        block = (a_col[rows, :] + b_row[...]) - 2.0 * cross[rows, :]
        acc = acc + fold(block * (u_ref[rows, :] * kern[rows, :] * v))
    total = group_sum(0, jnp.sum(acc, axis=0, keepdims=True))
    loss_ref[...] = jnp.broadcast_to(jnp.sum(total, axis=1, keepdims=True), loss_ref.shape)


def solution(mesh):
    grid_spec = P(("pairs", "rows"), "cols")
    n_rows, n_cols = mesh.shape["rows"], mesh.shape["cols"]

    def local_fn(c1_blk, c2_blk, t0_blk, p_blk, q_blk, eps_blk):
        height, width = t0_blk.shape
        full = width * n_cols
        n_chunk = width // LANES
        n_piece = c1_blk.shape[1] // PIECE
        n_steps = eps_blk.shape[0]
        vmem = pl.BlockSpec(memory_space=pltpu.VMEM)
        f32, b16, dma = jnp.float32, jnp.bfloat16, pltpu.SemaphoreType.DMA
        plan, loss = pl.pallas_call(
            functools.partial(gw_kernel, n_rows, n_cols, n_steps),
            out_shape=(jax.ShapeDtypeStruct((height, width), f32), jax.ShapeDtypeStruct((1, full), f32)),
            in_specs=[pl.BlockSpec(memory_space=pltpu.SMEM), pl.BlockSpec(memory_space=pl.ANY)] + [vmem] * 4,
            out_specs=(vmem, vmem),
            scratch_shapes=[
                pltpu.VMEM((n_cols * n_piece, height, PIECE), b16),
                pltpu.VMEM((n_rows, n_chunk, height, LANES), b16),
                pltpu.VMEM((2, n_cols, n_chunk, height, LANES), b16),
                pltpu.VMEM((n_chunk, height, LANES), f32),
                pltpu.VMEM((height, full), f32),
                pltpu.VMEM((height, full), f32),
                pltpu.VMEM((height, 1), f32),
                pltpu.VMEM((2, n_rows, 1, full), f32),
                pltpu.VMEM((2, height, PIECE), f32),
                pltpu.VMEM((height, LANES), f32),
                pltpu.VMEM((height, 1), f32),
                pltpu.VMEM((height, 1), f32),
                pltpu.VMEM((1, full), f32),
                pltpu.VMEM((1, full), f32),
                pltpu.VMEM((n_rows, n_cols) + c2_blk.shape, b16),
                pltpu.VMEM((full, full), b16),
                pltpu.VMEM((n_rows, 1, height), f32),
                pltpu.VMEM((n_cols, 1, width), f32),
                pltpu.VMEM((n_cols, 1, width), f32),
                pltpu.VMEM((n_rows, 1, width), f32),
                pltpu.VMEM((n_cols, 1, height), f32),
                dma((n_chunk, 14)), dma((n_rows, n_chunk, 2)),
                dma((n_chunk, 6)), dma((2, n_cols, n_chunk, 2)),
                dma((2, n_rows - 1)), dma((2, n_rows)),
                dma((3 * n_piece,)), dma((n_cols * n_piece,)),
                dma((7, n_rows)), dma((7, n_rows)), dma((2,)),
            ],
            compiler_params=pltpu.CompilerParams(collective_id=0, has_side_effects=True, vmem_limit_bytes=62 * 2**20),
        )(eps_blk, c1_blk, c2_blk, t0_blk, p_blk[None, :], q_blk[None, :])
        return plan, loss[0, :1]

    return jax.shard_map(local_fn, mesh=mesh, in_specs=(grid_spec, grid_spec, grid_spec, P(("pairs", "rows")), P(("pairs", "cols")), P("pairs")), out_specs=(grid_spec, P("pairs")), check_vma=False)
```

```python
import functools

import jax
import jax.numpy as jnp
from jax import lax
from jax.experimental import pallas as pl
from jax.experimental.pallas import tpu as pltpu
from jax.sharding import PartitionSpec as P

SWEEPS = 10
MESH = pl.DeviceIdType.MESH
BLK = 128
LANES = 128
PIECE = 256
N_PART = 1


def gw_kernel(n_rows, n_cols, n_steps, n_part, eps_ref, c1_ref, c2_ref, t0_ref, p_ref, q_ref,
              t_ref, loss_ref, c1s, tp, ap, lead, cross, kern, u_ref, row_sum, red,
              stage, a_acc, a_col, p_col, b_row, q_row, c2f, c2s, p_all, q_all, b_all, b_red, a_red,
              t_send, t_recv, a_send, a_recv, s_send, s_recv, c_send, c_recv, x_send, x_recv, ld_sem):
    me_r = lax.axis_index("rows")
    me_c = lax.axis_index("cols")
    chip, core = me_r // 2, me_r % 2
    n_chips = n_rows // 2
    height, width = t0_ref.shape
    half = height // 2
    n_chunk = width // LANES
    n_piece = c1_ref.shape[1] // PIECE
    per_slot = height // PIECE
    n_blk = height // BLK

    def row_id(chip_off, core_sel):
        return ((chip + chip_off + n_chips) % n_chips) * 2 + core_sel

    sib = row_id(0, 1 - core)
    right, left, far = row_id(1, core), row_id(-1, core), row_id(2, core)
    up, down, opp = (me_c + 1) % n_cols, (me_c + n_cols - 1) % n_cols, (me_c + 2) % n_cols

    barrier = pltpu.get_barrier_semaphore()
    for d in range(1, n_rows):
        pl.semaphore_signal(barrier, inc=1, device_id={"rows": (me_r + d) % n_rows}, device_id_type=MESH)
    for d in range(1, n_cols):
        pl.semaphore_signal(barrier, inc=1, device_id={"cols": (me_c + d) % n_cols}, device_id_type=MESH)
    pl.semaphore_wait(barrier, n_rows + n_cols - 2)

    def share(idx, axis, ref_of):
        me, n = (me_r, n_rows) if axis == "rows" else (me_c, n_cols)

        def copy(slot, d):
            return pltpu.make_async_remote_copy(src_ref=ref_of(slot), dst_ref=ref_of(slot), send_sem=x_send.at[idx, d],
                                                recv_sem=x_recv.at[idx, slot], device_id={axis: (me + d) % n}, device_id_type=MESH)

        for d in range(1, n):
            copy(me, d).start()

        def finish():
            for d in range(1, n):
                copy((me + d) % n, d).wait_recv()
            for d in range(1, n):
                copy(me, d).wait_send()

        return finish

    part_w = kern.shape[1] // n_part

    def sum_copy(par, h, ref, d):
        return pltpu.make_async_remote_copy(src_ref=ref, dst_ref=ref, send_sem=s_send.at[par, h], recv_sem=s_recv.at[par, h],
                                            device_id={"rows": (me_r + d) % n_rows}, device_id_type=MESH)

    def push(par, h, value):
        red[par, h, me_r] = value
        for d in range(1, n_rows):
            sum_copy(par, h, red.at[par, h, me_r], d).start()

    def pull(par, h):
        every = sum_copy(par, h, red.at[par, h, pl.ds(0, n_rows - 1)], 1)
        every.wait_recv()
        total = red[par, h, 0]
        for d in range(1, n_rows):
            total = total + red[par, h, d]
        every.wait_send()
        return total

    def t_copy(slot, chunk, part, target, send_idx):
        ref = tp.at[slot, chunk, pl.ds(part * half, half)]
        return pltpu.make_async_remote_copy(src_ref=ref, dst_ref=ref, send_sem=t_send.at[chunk, send_idx],
                                            recv_sem=t_recv.at[slot, chunk, part], device_id={"rows": target}, device_id_type=MESH)

    t_sent = []

    def t_push(slot, chunk, part, target, send_idx):
        copy = t_copy(slot, chunk, part, target, send_idx)
        copy.start()
        t_sent.append(copy)

    def t_take(slot, chunk, part):
        t_copy(slot, chunk, part, sib, 0).wait_recv()

    def t_start(chunk):
        for part in (0, 1):
            t_push(me_r, chunk, part, right, part)
            t_push(me_r, chunk, 1 - part, left, 2 + part)
        for part in (0, 1):
            t_push(me_r, chunk, part, sib, 4 + part)

    def t_near(chunk):
        t_take(left, chunk, 0)
        t_push(left, chunk, 0, right, 6)
        t_take(right, chunk, 1)
        t_push(right, chunk, 1, left, 7)
        t_push(left, chunk, 0, sib, 8)
        t_push(right, chunk, 1, sib, 9)

    def t_rest(chunk):
        t_take(left, chunk, 1)
        t_push(left, chunk, 1, sib, 10)
        t_take(right, chunk, 0)
        t_push(right, chunk, 0, sib, 11)

    def t_far(chunk):
        for part in (0, 1):
            t_take(far, chunk, part)
            t_push(far, chunk, part, sib, 12 + part)

    def t_sib(chunk, chip_off):
        slot = row_id(chip_off, 1 - core)
        t_take(slot, chunk, 0)
        t_take(slot, chunk, 1)
        return slot

    def t_done():
        for copy in t_sent:
            copy.wait_send()
        t_sent.clear()

    def a_copy(par, slot, chunk, part, target, send_idx):
        ref = ap.at[par, slot, chunk, pl.ds(part * half, half)]
        return pltpu.make_async_remote_copy(src_ref=ref, dst_ref=ref, send_sem=a_send.at[chunk, send_idx],
                                            recv_sem=a_recv.at[par, slot, chunk, part], device_id={"cols": target}, device_id_type=MESH)

    a_sent = []

    def a_push(par, slot, chunk, part, target, send_idx):
        copy = a_copy(par, slot, chunk, part, target, send_idx)
        copy.start()
        a_sent.append(copy)

    def a_take(par, slot, chunk, part):
        a_copy(par, slot, chunk, part, up, 0).wait_recv()

    def a_start(par, chunk):
        ap[par, me_c, chunk] = lead[chunk].astype(jnp.bfloat16)
        for part in (0, 1):
            a_push(par, me_c, chunk, part, up, part)
            a_push(par, me_c, chunk, 1 - part, down, 2 + part)

    def a_near(par, chunk):
        a_take(par, down, chunk, 0)
        a_push(par, down, chunk, 0, up, 4)
        a_take(par, up, chunk, 1)
        a_push(par, up, chunk, 1, down, 5)

    def a_rest(par, chunk):
        a_take(par, down, chunk, 1)
        a_take(par, up, chunk, 0)

    def a_far(par, chunk):
        a_take(par, opp, chunk, 0)
        a_take(par, opp, chunk, 1)

    def a_done():
        for copy in a_sent:
            copy.wait_send()
        a_sent.clear()

    def c1_slot(slot):
        return jnp.concatenate([c1s[slot * per_slot + j] for j in range(per_slot)], axis=1)

    def lead_add(slot, chunk, part=None, first=False):
        if part is None:
            prod = jnp.dot(c1_slot(slot), tp[slot, chunk], preferred_element_type=jnp.float32)
        else:
            hop = per_slot // 2
            block = jnp.concatenate([c1s[slot * per_slot + part * hop + j] for j in range(hop)], axis=1)
            prod = jnp.dot(block, tp[slot, chunk, part * half:(part + 1) * half], preferred_element_type=jnp.float32)
        lead[chunk] = prod if first else lead[chunk] + prod

    def lead_both(slot):
        plan = jnp.concatenate([tp[slot, k] for k in range(n_chunk)], axis=1)
        prod = jnp.dot(c1_slot(slot), plan, preferred_element_type=jnp.float32)
        for k in range(n_chunk):
            lead[k] = lead[k] + prod[:, k * LANES:(k + 1) * LANES]

    def cross_add(par, pairs, first=False):
        block = jnp.concatenate([ap[par, slot, k] for slot, k in pairs], axis=1)
        rows = [pl.ds(pl.multiple_of(slot * width + k * LANES, LANES), LANES) for slot, k in pairs]
        right_side = jnp.concatenate([c2s[r, :] for r in rows], axis=0)
        prod = jnp.dot(block, right_side, preferred_element_type=jnp.float32)
        cross[...] = prod if first else cross[...] + prod

    def whole(slot):
        return [(slot, k) for k in range(n_chunk)]

    def piece_load(i):
        cols = pl.ds(pl.multiple_of(i * PIECE, PIECE), PIECE)
        return pltpu.make_async_copy(c1_ref.at[:, cols], stage.at[i % 2], ld_sem.at[i % 2])

    def piece_copy(piece, target, send_idx):
        return pltpu.make_async_remote_copy(src_ref=c1s.at[piece], dst_ref=c1s.at[piece], send_sem=c_send.at[send_idx],
                                            recv_sem=c_recv.at[piece], device_id={"cols": target}, device_id_type=MESH)

    def prologue():
        piece_load(0).start()
        p_all[me_r] = p_ref[...]
        p_fin = share(0, "rows", lambda s: p_all.at[s])
        q_all[me_c] = q_ref[...]
        q_fin = share(1, "cols", lambda s: q_all.at[s])
        c2f[me_r, me_c] = c2_ref[...].astype(jnp.bfloat16)
        c2y_fin = share(2, "cols", lambda s: c2f.at[me_r, s])
        for k in range(n_chunk):
            tp[me_r, k] = t0_ref[:, k * LANES:(k + 1) * LANES].astype(jnp.bfloat16)
        for k in range(n_chunk):
            t_start(k)
        a_acc[...] = jnp.zeros_like(a_acc)
        p_fin()

        def own_piece(i, carry):
            piece_load(i).wait()

            @pl.when(i + 1 < n_piece)
            def _():
                piece_load(i + 1).start()

            block = stage[i % 2]
            piece = me_c * n_piece + i
            c1s[piece] = block.astype(jnp.bfloat16)
            piece_copy(piece, up, i).start()
            piece_copy(piece, down, n_piece + i).start()
            where = piece * PIECE
            p_row = p_all[where // height, :, pl.ds(pl.multiple_of(where % height, PIECE), PIECE)]
            sq = block * block * p_row
            acc = a_acc[...]
            for k in range(PIECE // LANES):
                acc = acc + sq[:, k * LANES:(k + 1) * LANES]
            a_acc[...] = acc
            return carry

        lax.fori_loop(0, n_piece, own_piece, 0)
        q_fin()
        q_row[...] = jnp.concatenate([q_all[k] for k in range(n_cols)], axis=1)
        a_red[me_c] = jnp.sum(a_acc[...].T, axis=0, keepdims=True)
        a_fin = share(3, "cols", lambda s: a_red.at[s])
        low = me_r * c2_ref.shape[0]
        q_piece = q_all[low // width, :, pl.ds(pl.multiple_of(low % width, LANES), LANES)]
        q_col = jnp.broadcast_to(q_piece, (LANES, LANES)).T
        sq = c2_ref[...] * c2_ref[...]
        b_red[me_r] = jnp.sum(sq * q_col[:, :1], axis=0, keepdims=True)
        b_fin = share(4, "rows", lambda s: b_red.at[s])
        p_col[...] = jnp.broadcast_to(p_ref[...], (LANES, height)).T[:, :1]
        c2y_fin()
        c2x_fin = share(5, "rows", lambda s: c2f.at[s])
        for k in range(n_chunk):
            t_near(k)
        for k in range(n_chunk):
            t_rest(k)
        b_fin()
        total = b_red[0]
        for s in range(1, n_rows):
            total = total + b_red[s]
        b_all[me_c] = total
        ball_fin = share(6, "cols", lambda s: b_all.at[s])
        for k in range(n_chunk):
            t_far(k)
        for k in range(n_chunk):
            for off in (0, -1, 1, 2):
                t_sib(k, off)
        t_done()
        lead[...] = jnp.zeros_like(lead)

        def group(which):
            def body(j, carry):
                lead_both(which * (n_piece // per_slot) + j)
                return carry

            lax.fori_loop(0, n_piece // per_slot, body, 0)

        group(me_c)
        hop = n_piece // 2
        for i in range(n_piece):
            piece_copy(down * n_piece + i, up, 0).wait_recv()
            if i < hop:
                piece_copy(down * n_piece + i, up, 2 * n_piece + i).start()
            piece_copy(up * n_piece + i, up, 0).wait_recv()
            if i >= hop:
                piece_copy(up * n_piece + i, down, 2 * n_piece + i).start()
        group(down)
        group(up)
        a_fin()
        total = a_red[0]
        for s in range(1, n_cols):
            total = total + a_red[s]
        a_col[...] = jnp.broadcast_to(total, (LANES, height)).T[:, :1]
        ball_fin()
        b_row[...] = jnp.concatenate([b_all[k] for k in range(n_cols)], axis=1)
        c2x_fin()
        depth = c2_ref.shape[0]
        for r in range(n_rows):
            for c in range(n_cols):
                c2s[r * depth:(r + 1) * depth, c * width:(c + 1) * width] = c2f[r, c]
        for i in range(n_piece):
            piece_copy(opp * n_piece + i, up, 0).wait_recv()
        group(opp)
        for i in range(n_piece):
            piece_copy(me_c * n_piece + i, up, i).wait_send()
            piece_copy(me_c * n_piece + i, down, n_piece + i).wait_send()
            if i < hop:
                piece_copy(down * n_piece + i, up, 2 * n_piece + i).wait_send()
            else:
                piece_copy(up * n_piece + i, down, 2 * n_piece + i).wait_send()

        for k in range(n_chunk):
            a_start(0, k)
        cross_add(0, whole(me_c), True)
        for k in range(n_chunk):
            a_near(0, k)
        for k in range(n_chunk):
            a_rest(0, k)
        cross_add(0, whole(down))
        cross_add(0, whole(up))
        for k in range(n_chunk):
            a_far(0, k)
        cross_add(0, whole(opp))
        a_done()

    def t_sib_part(chunk, chip_off, part):
        slot = row_id(chip_off, 1 - core)
        t_take(slot, chunk, part)
        lead_add(slot, chunk, part)

    def cost(par):
        def near(chunk):
            lead_add(left, chunk, 0)
            lead_add(right, chunk, 1)
            t_sib_part(chunk, -1, 0)
            t_sib_part(chunk, 1, 1)

        def rest(chunk):
            t_rest(chunk)
            lead_add(left, chunk, 1)
            lead_add(right, chunk, 0)
            t_sib_part(chunk, -1, 1)
            t_sib_part(chunk, 1, 0)

        def late(chunk):
            t_far(chunk)
            lead_add(far, chunk)
            lead_add(t_sib(chunk, 2), chunk)
            a_start(par, chunk)

        lead_add(me_r, 0, None, True)
        lead_add(t_sib(0, 0), 0)
        t_near(0)
        t_start(1)
        near(0)
        lead_add(me_r, 1, None, True)
        lead_add(t_sib(1, 0), 1)
        rest(0)
        late(0)
        t_near(1)
        near(1)
        rest(1)
        a_near(par, 0)
        late(1)
        a_rest(par, 0)
        cross_add(par, whole(me_c), True)
        cross_add(par, [(down, 0), (up, 0)])
        a_far(par, 0)
        cross_add(par, [(opp, 0)])
        a_near(par, 1)
        a_rest(par, 1)
        cross_add(par, [(down, 1), (up, 1)])
        a_far(par, 1)
        cross_add(par, [(opp, 1)])
        t_done()
        a_done()

    def fold(block):
        return jnp.sum(block.reshape(BLK // 8, 8, block.shape[1]), axis=0)

    def part_cols(h):
        return slice(h * part_w, (h + 1) * part_w)

    def row_lanes(block, weight):
        total = None
        for j in range(block.shape[1] // LANES):
            cols = slice(j * LANES, (j + 1) * LANES)
            term = block[:, cols] if weight is None else block[:, cols] * weight[:, cols]
            total = term if total is None else total + term
        return total

    def push_part(par, h):
        acc = jnp.zeros((8, part_w), jnp.float32)
        for k in range(n_blk):
            rows = pl.ds(k * BLK, BLK)
            acc = acc + fold(kern[rows, part_cols(h)] * u_ref[rows, :])
        push(par, h, jnp.sum(acc, axis=0, keepdims=True))

    def first_sweep(step):
        inv_eps = 1.0 / jnp.full((1, 1), eps_ref[step], jnp.float32)
        for k in range(n_blk):
            rows = pl.ds(k * BLK, BLK)
            block = (a_col[rows, :] + b_row[...]) - 2.0 * cross[rows, :]
            low = jnp.min(block, axis=1, keepdims=True)
            block = jnp.exp((low - block) * inv_eps)
            kern[rows, :] = block
            u_ref[rows, :] = p_col[rows, :] / jnp.sum(row_lanes(block, None), axis=1, keepdims=True)
        for h in range(n_part):
            push_part(0, h)

    def scale(par, h):
        return q_row[:, part_cols(h)] / pull(par, h)

    def sweep(i, carry):
        prev, cur = (i + 1) % 2, i % 2
        for h in range(n_part - 1):
            v = scale(prev, h)
            for k in range(n_blk):
                rows = pl.ds(k * BLK, BLK)
                lanes = row_lanes(kern[rows, part_cols(h)], v)
                row_sum[rows, :] = lanes if h == 0 else row_sum[rows, :] + lanes
        h = n_part - 1
        v = scale(prev, h)
        acc = jnp.zeros((8, part_w), jnp.float32)
        for k in range(n_blk):
            rows = pl.ds(k * BLK, BLK)
            lanes = row_sum[rows, :] + row_lanes(kern[rows, part_cols(h)], v)
            u = p_col[rows, :] / jnp.sum(lanes, axis=1, keepdims=True)
            u_ref[rows, :] = u
            acc = acc + fold(kern[rows, part_cols(0)] * u)
        push(cur, 0, jnp.sum(acc, axis=0, keepdims=True))
        for h in range(1, n_part):
            push_part(cur, h)
        return carry

    v_ref = loss_ref

    def outer(step, carry):
        first_sweep(step)
        lax.fori_loop(1, SWEEPS, sweep, 0)
        for h in range(n_part):
            v_ref[:, part_cols(h)] = scale((SWEEPS - 1) % 2, h)
        for c in range(n_chunk):
            cols = pl.ds(pl.multiple_of(me_c * width + c * LANES, LANES), LANES)
            for k in range(n_blk):
                rows = pl.ds(k * BLK, BLK)
                plan = u_ref[rows, :] * kern[rows, cols] * v_ref[:, cols]
                t_ref[rows, c * LANES:(c + 1) * LANES] = plan
                tp[me_r, c, rows, :] = plan.astype(jnp.bfloat16)
            if c == 0:
                t_start(0)
        cost((step + 1) % 2)
        return carry

    prologue()
    lax.fori_loop(0, n_steps, outer, 0)

    v = v_ref[...]
    acc = jnp.zeros((8, v.shape[1]), jnp.float32)
    for k in range(n_blk):
        rows = pl.ds(k * BLK, BLK)
        block = (a_col[rows, :] + b_row[...]) - 2.0 * cross[rows, :]
        acc = acc + fold(block * (u_ref[rows, :] * kern[rows, :] * v))
    total = jnp.sum(acc, axis=0, keepdims=True)
    half_sum = total[:, part_cols(0)]
    for h in range(1, n_part):
        half_sum = half_sum + total[:, part_cols(h)]
    push(SWEEPS % 2, 0, half_sum)
    loss_ref[...] = jnp.broadcast_to(jnp.sum(pull(SWEEPS % 2, 0), axis=1, keepdims=True), loss_ref.shape)


def solution(mesh):
    grid_spec = P(("pairs", "rows"), "cols")
    n_rows, n_cols = mesh.shape["rows"], mesh.shape["cols"]

    def local_fn(c1_blk, c2_blk, t0_blk, p_blk, q_blk, eps_blk):
        height, width = t0_blk.shape
        full = width * n_cols
        n_chunk = width // LANES
        n_piece = c1_blk.shape[1] // PIECE
        n_steps = eps_blk.shape[0]
        vmem = pl.BlockSpec(memory_space=pltpu.VMEM)
        f32, b16, dma = jnp.float32, jnp.bfloat16, pltpu.SemaphoreType.DMA
        plan, loss = pl.pallas_call(
            functools.partial(gw_kernel, n_rows, n_cols, n_steps, N_PART),
            out_shape=(jax.ShapeDtypeStruct((height, width), f32), jax.ShapeDtypeStruct((1, full), f32)),
            in_specs=[pl.BlockSpec(memory_space=pltpu.SMEM), pl.BlockSpec(memory_space=pl.ANY)] + [vmem] * 4,
            out_specs=(vmem, vmem),
            scratch_shapes=[
                pltpu.VMEM((n_cols * n_piece, height, PIECE), b16),
                pltpu.VMEM((n_rows, n_chunk, height, LANES), b16),
                pltpu.VMEM((2, n_cols, n_chunk, height, LANES), b16),
                pltpu.VMEM((n_chunk, height, LANES), f32),
                pltpu.VMEM((height, full), f32),
                pltpu.VMEM((height, full), f32),
                pltpu.VMEM((height, 1), f32),
                pltpu.VMEM((height, LANES), f32),
                pltpu.VMEM((2, N_PART, n_rows, 1, full // N_PART), f32),
                pltpu.VMEM((2, height, PIECE), f32),
                pltpu.VMEM((height, LANES), f32),
                pltpu.VMEM((height, 1), f32),
                pltpu.VMEM((height, 1), f32),
                pltpu.VMEM((1, full), f32),
                pltpu.VMEM((1, full), f32),
                pltpu.VMEM((n_rows, n_cols) + c2_blk.shape, b16),
                pltpu.VMEM((full, full), b16),
                pltpu.VMEM((n_rows, 1, height), f32),
                pltpu.VMEM((n_cols, 1, width), f32),
                pltpu.VMEM((n_cols, 1, width), f32),
                pltpu.VMEM((n_rows, 1, width), f32),
                pltpu.VMEM((n_cols, 1, height), f32),
                dma((n_chunk, 14)), dma((n_rows, n_chunk, 2)),
                dma((n_chunk, 6)), dma((2, n_cols, n_chunk, 2)),
                dma((2, N_PART)), dma((2, N_PART)),
                dma((3 * n_piece,)), dma((n_cols * n_piece,)),
                dma((7, n_rows)), dma((7, n_rows)), dma((2,)),
            ],
            compiler_params=pltpu.CompilerParams(collective_id=0, has_side_effects=True, vmem_limit_bytes=62 * 2**20),
        )(eps_blk, c1_blk, c2_blk, t0_blk, p_blk[None, :], q_blk[None, :])
        return plan, loss[0, :1]

    return jax.shard_map(local_fn, mesh=mesh, in_specs=(grid_spec, grid_spec, grid_spec, P(("pairs", "rows")), P(("pairs", "cols")), P("pairs")), out_specs=(grid_spec, P("pairs")), check_vma=False)
```

```python
import functools

import jax
import jax.numpy as jnp
from jax import lax
from jax.experimental import pallas as pl
from jax.experimental.pallas import tpu as pltpu
from jax.sharding import PartitionSpec as P

SWEEPS = 10
MESH = pl.DeviceIdType.MESH
BLK = 128
LANES = 128
PIECE = 256
N_PART = 1


def gw_kernel(n_rows, n_cols, n_steps, n_part, eps_ref, c1_ref, c2_ref, t0_ref, p_ref, q_ref,
              t_ref, loss_ref, c1s, tp, ap, lead, cross, kern, u_ref, row_sum, red,
              stage, a_acc, a_col, p_col, b_row, q_row, c2f, c2s, p_all, q_all, b_all, b_red, a_red,
              t_send, t_recv, a_send, a_recv, s_send, s_recv, c_send, c_recv, x_send, x_recv, ld_sem):
    me_r = lax.axis_index("rows")
    me_c = lax.axis_index("cols")
    chip, core = me_r // 2, me_r % 2
    n_chips = n_rows // 2
    height, width = t0_ref.shape
    half = height // 2
    n_chunk = width // LANES
    n_piece = c1_ref.shape[1] // PIECE
    per_slot = height // PIECE
    n_blk = height // BLK

    def row_id(chip_off, core_sel):
        return ((chip + chip_off + n_chips) % n_chips) * 2 + core_sel

    sib = row_id(0, 1 - core)
    right, left, far = row_id(1, core), row_id(-1, core), row_id(2, core)
    up, down, opp = (me_c + 1) % n_cols, (me_c + n_cols - 1) % n_cols, (me_c + 2) % n_cols

    first_load = pltpu.make_async_copy(c1_ref.at[:, pl.ds(0, PIECE)], stage.at[0], ld_sem.at[0])
    first_load.start()
    barrier = pltpu.get_barrier_semaphore()
    for d in range(1, n_rows):
        pl.semaphore_signal(barrier, inc=1, device_id={"rows": (me_r + d) % n_rows}, device_id_type=MESH)
    for d in range(1, n_cols):
        pl.semaphore_signal(barrier, inc=1, device_id={"cols": (me_c + d) % n_cols}, device_id_type=MESH)
    pl.semaphore_wait(barrier, n_rows + n_cols - 2)

    def share(idx, axis, ref_of):
        me, n = (me_r, n_rows) if axis == "rows" else (me_c, n_cols)

        def copy(slot, d):
            return pltpu.make_async_remote_copy(src_ref=ref_of(slot), dst_ref=ref_of(slot), send_sem=x_send.at[idx, d],
                                                recv_sem=x_recv.at[idx, slot], device_id={axis: (me + d) % n}, device_id_type=MESH)

        for d in range(1, n):
            copy(me, d).start()

        def finish():
            for d in range(1, n):
                copy((me + d) % n, d).wait_recv()
            for d in range(1, n):
                copy(me, d).wait_send()

        return finish

    part_w = kern.shape[1] // n_part

    peers = [far, row_id(2, 1 - core), left, right, row_id(-1, 1 - core), row_id(1, 1 - core), sib]

    def sum_copy(par, h, ref, target):
        return pltpu.make_async_remote_copy(src_ref=ref, dst_ref=ref, send_sem=s_send.at[par, h], recv_sem=s_recv.at[par, h],
                                            device_id={"rows": target}, device_id_type=MESH)

    def push(par, h, value):
        red[par, h, me_r] = value
        for target in peers:
            sum_copy(par, h, red.at[par, h, me_r], target).start()

    def pull(par, h):
        every = sum_copy(par, h, red.at[par, h, pl.ds(0, n_rows - 1)], sib)
        every.wait_recv()
        total = red[par, h, 0]
        for d in range(1, n_rows):
            total = total + red[par, h, d]
        every.wait_send()
        return total

    def t_copy(slot, chunk, part, target, send_idx):
        ref = tp.at[slot, chunk, pl.ds(part * half, half)]
        return pltpu.make_async_remote_copy(src_ref=ref, dst_ref=ref, send_sem=t_send.at[chunk, send_idx],
                                            recv_sem=t_recv.at[slot, chunk, part], device_id={"rows": target}, device_id_type=MESH)

    t_sent = []

    def t_push(slot, chunk, part, target, send_idx):
        copy = t_copy(slot, chunk, part, target, send_idx)
        copy.start()
        t_sent.append(copy)

    def t_take(slot, chunk, part):
        t_copy(slot, chunk, part, sib, 0).wait_recv()

    def t_start(chunk):
        for part in (0, 1):
            t_push(me_r, chunk, part, right, part)
            t_push(me_r, chunk, 1 - part, left, 2 + part)
        for part in (0, 1):
            t_push(me_r, chunk, part, sib, 4 + part)

    def t_near(chunk):
        t_take(left, chunk, 0)
        t_push(left, chunk, 0, right, 6)
        t_take(right, chunk, 1)
        t_push(right, chunk, 1, left, 7)
        t_push(left, chunk, 0, sib, 8)
        t_push(right, chunk, 1, sib, 9)

    def t_rest(chunk):
        t_take(left, chunk, 1)
        t_push(left, chunk, 1, sib, 10)
        t_take(right, chunk, 0)
        t_push(right, chunk, 0, sib, 11)

    def t_far(chunk):
        for part in (0, 1):
            t_take(far, chunk, part)
            t_push(far, chunk, part, sib, 12 + part)

    def t_sib(chunk, chip_off):
        slot = row_id(chip_off, 1 - core)
        t_take(slot, chunk, 0)
        t_take(slot, chunk, 1)
        return slot

    def t_done():
        for copy in t_sent:
            copy.wait_send()
        t_sent.clear()

    def a_copy(par, slot, chunk, part, target, send_idx):
        ref = ap.at[par, slot, chunk, pl.ds(part * half, half)]
        return pltpu.make_async_remote_copy(src_ref=ref, dst_ref=ref, send_sem=a_send.at[chunk, send_idx],
                                            recv_sem=a_recv.at[par, slot, chunk, part], device_id={"cols": target}, device_id_type=MESH)

    a_sent = []

    def a_push(par, slot, chunk, part, target, send_idx):
        copy = a_copy(par, slot, chunk, part, target, send_idx)
        copy.start()
        a_sent.append(copy)

    def a_take(par, slot, chunk, part):
        a_copy(par, slot, chunk, part, up, 0).wait_recv()

    def a_start(par, chunk):
        ap[par, me_c, chunk] = lead[chunk].astype(jnp.bfloat16)
        for part in (0, 1):
            a_push(par, me_c, chunk, part, up, part)
            a_push(par, me_c, chunk, 1 - part, down, 2 + part)

    def a_near(par, chunk):
        a_take(par, down, chunk, 0)
        a_push(par, down, chunk, 0, up, 4)
        a_take(par, up, chunk, 1)
        a_push(par, up, chunk, 1, down, 5)

    def a_rest(par, chunk):
        a_take(par, down, chunk, 1)
        a_take(par, up, chunk, 0)

    def a_far(par, chunk):
        a_take(par, opp, chunk, 0)
        a_take(par, opp, chunk, 1)

    def a_done():
        for copy in a_sent:
            copy.wait_send()
        a_sent.clear()

    def c1_slot(slot):
        return jnp.concatenate([c1s[slot * per_slot + j] for j in range(per_slot)], axis=1)

    def lead_add(slot, chunk, part=None, first=False):
        if part is None:
            prod = jnp.dot(c1_slot(slot), tp[slot, chunk], preferred_element_type=jnp.float32)
        else:
            hop = per_slot // 2
            block = jnp.concatenate([c1s[slot * per_slot + part * hop + j] for j in range(hop)], axis=1)
            prod = jnp.dot(block, tp[slot, chunk, part * half:(part + 1) * half], preferred_element_type=jnp.float32)
        lead[chunk] = prod if first else lead[chunk] + prod

    def lead_both(slot):
        plan = jnp.concatenate([tp[slot, k] for k in range(n_chunk)], axis=1)
        prod = jnp.dot(c1_slot(slot), plan, preferred_element_type=jnp.float32)
        for k in range(n_chunk):
            lead[k] = lead[k] + prod[:, k * LANES:(k + 1) * LANES]

    def cross_add(par, pairs, first=False):
        block = jnp.concatenate([ap[par, slot, k] for slot, k in pairs], axis=1)
        rows = [pl.ds(pl.multiple_of(slot * width + k * LANES, LANES), LANES) for slot, k in pairs]
        right_side = jnp.concatenate([c2s[r, :] for r in rows], axis=0)
        prod = jnp.dot(block, right_side, preferred_element_type=jnp.float32)
        cross[...] = prod if first else cross[...] + prod

    def whole(slot):
        return [(slot, k) for k in range(n_chunk)]

    def piece_load(i):
        cols = pl.ds(pl.multiple_of(i * PIECE, PIECE), PIECE)
        return pltpu.make_async_copy(c1_ref.at[:, cols], stage.at[i % 2], ld_sem.at[i % 2])

    def piece_copy(piece, target, send_idx):
        return pltpu.make_async_remote_copy(src_ref=c1s.at[piece], dst_ref=c1s.at[piece], send_sem=c_send.at[send_idx],
                                            recv_sem=c_recv.at[piece], device_id={"cols": target}, device_id_type=MESH)

    def prologue():
        p_all[me_r] = p_ref[...]
        p_fin = share(0, "rows", lambda s: p_all.at[s])
        q_all[me_c] = q_ref[...]
        q_fin = share(1, "cols", lambda s: q_all.at[s])
        c2f[me_r, me_c] = c2_ref[...].astype(jnp.bfloat16)
        c2y_fin = share(2, "cols", lambda s: c2f.at[me_r, s])
        for k in range(n_chunk):
            tp[me_r, k] = t0_ref[:, k * LANES:(k + 1) * LANES].astype(jnp.bfloat16)
        for k in range(n_chunk):
            t_start(k)
        a_acc[...] = jnp.zeros_like(a_acc)
        p_fin()

        def own_piece(i, carry):
            piece_load(i).wait()

            @pl.when(i + 1 < n_piece)
            def _():
                piece_load(i + 1).start()

            block = stage[i % 2]
            piece = me_c * n_piece + i
            c1s[piece] = block.astype(jnp.bfloat16)
            piece_copy(piece, up, i).start()
            piece_copy(piece, down, n_piece + i).start()
            where = piece * PIECE
            p_row = p_all[where // height, :, pl.ds(pl.multiple_of(where % height, PIECE), PIECE)]
            sq = block * block * p_row
            acc = a_acc[...]
            for k in range(PIECE // LANES):
                acc = acc + sq[:, k * LANES:(k + 1) * LANES]
            a_acc[...] = acc
            return carry

        lax.fori_loop(0, n_piece, own_piece, 0)
        q_fin()
        q_row[...] = jnp.concatenate([q_all[k] for k in range(n_cols)], axis=1)
        a_red[me_c] = jnp.sum(a_acc[...].T, axis=0, keepdims=True)
        a_fin = share(3, "cols", lambda s: a_red.at[s])
        low = me_r * c2_ref.shape[0]
        q_piece = q_all[low // width, :, pl.ds(pl.multiple_of(low % width, LANES), LANES)]
        q_col = jnp.broadcast_to(q_piece, (LANES, LANES)).T
        sq = c2_ref[...] * c2_ref[...]
        b_red[me_r] = jnp.sum(sq * q_col[:, :1], axis=0, keepdims=True)
        b_fin = share(4, "rows", lambda s: b_red.at[s])
        p_col[...] = jnp.broadcast_to(p_ref[...], (LANES, height)).T
        c2y_fin()
        c2x_fin = share(5, "rows", lambda s: c2f.at[s])
        for k in range(n_chunk):
            t_near(k)
        for k in range(n_chunk):
            t_rest(k)
        b_fin()
        total = b_red[0]
        for s in range(1, n_rows):
            total = total + b_red[s]
        b_all[me_c] = total
        ball_fin = share(6, "cols", lambda s: b_all.at[s])
        for k in range(n_chunk):
            t_far(k)
        for k in range(n_chunk):
            for off in (0, -1, 1, 2):
                t_sib(k, off)
        t_done()
        lead[...] = jnp.zeros_like(lead)

        def group(which):
            def body(j, carry):
                lead_both(which * (n_piece // per_slot) + j)
                return carry

            lax.fori_loop(0, n_piece // per_slot, body, 0)

        group(me_c)
        hop = n_piece // 2
        for i in range(n_piece):
            piece_copy(down * n_piece + i, up, 0).wait_recv()
            if i < hop:
                piece_copy(down * n_piece + i, up, 2 * n_piece + i).start()
            piece_copy(up * n_piece + i, up, 0).wait_recv()
            if i >= hop:
                piece_copy(up * n_piece + i, down, 2 * n_piece + i).start()
        group(down)
        group(up)
        a_fin()
        total = a_red[0]
        for s in range(1, n_cols):
            total = total + a_red[s]
        a_col[...] = jnp.broadcast_to(total, (LANES, height)).T
        ball_fin()
        b_row[...] = jnp.concatenate([b_all[k] for k in range(n_cols)], axis=1)
        c2x_fin()
        depth = c2_ref.shape[0]
        for r in range(n_rows):
            for c in range(n_cols):
                c2s[r * depth:(r + 1) * depth, c * width:(c + 1) * width] = c2f[r, c]
        for i in range(n_piece):
            piece_copy(opp * n_piece + i, up, 0).wait_recv()
        group(opp)
        for i in range(n_piece):
            piece_copy(me_c * n_piece + i, up, i).wait_send()
            piece_copy(me_c * n_piece + i, down, n_piece + i).wait_send()
            if i < hop:
                piece_copy(down * n_piece + i, up, 2 * n_piece + i).wait_send()
            else:
                piece_copy(up * n_piece + i, down, 2 * n_piece + i).wait_send()

        for k in range(n_chunk):
            a_start(0, k)
        cross_add(0, whole(me_c), True)
        for k in range(n_chunk):
            a_near(0, k)
        for k in range(n_chunk):
            a_rest(0, k)
        cross_add(0, whole(down))
        cross_add(0, whole(up))
        for k in range(n_chunk):
            a_far(0, k)
        cross_add(0, whole(opp))
        a_done()

    def t_sib_part(chunk, chip_off, part):
        slot = row_id(chip_off, 1 - core)
        t_take(slot, chunk, part)
        lead_add(slot, chunk, part)

    def cost(par):
        def near(chunk):
            lead_add(left, chunk, 0)
            lead_add(right, chunk, 1)
            t_sib_part(chunk, -1, 0)
            t_sib_part(chunk, 1, 1)

        def rest(chunk):
            t_rest(chunk)
            lead_add(left, chunk, 1)
            lead_add(right, chunk, 0)
            t_sib_part(chunk, -1, 1)
            t_sib_part(chunk, 1, 0)

        def late(chunk):
            t_far(chunk)
            lead_add(far, chunk)
            lead_add(t_sib(chunk, 2), chunk)
            a_start(par, chunk)

        lead_add(me_r, 0, None, True)
        lead_add(t_sib(0, 0), 0)
        t_near(0)
        t_start(1)
        near(0)
        lead_add(me_r, 1, None, True)
        lead_add(t_sib(1, 0), 1)
        rest(0)
        late(0)
        t_near(1)
        near(1)
        rest(1)
        a_near(par, 0)
        late(1)
        a_rest(par, 0)
        cross_add(par, whole(me_c), True)
        cross_add(par, [(down, 0), (up, 0)])
        a_far(par, 0)
        cross_add(par, [(opp, 0)])
        a_near(par, 1)
        a_rest(par, 1)
        cross_add(par, [(down, 1), (up, 1)])
        a_far(par, 1)
        cross_add(par, [(opp, 1)])
        t_done()
        a_done()

    def fold(block):
        return jnp.sum(block.reshape(BLK // 8, 8, block.shape[1]), axis=0)

    def part_cols(h):
        return slice(h * part_w, (h + 1) * part_w)

    def lane_tiles(ref, rows, cols):
        return [ref[rows, j:j + LANES] for j in range(cols.start, cols.stop, LANES)]

    def row_sums(tiles):
        total = tiles[0]
        for tile in tiles[1:]:
            total = total + tile
        return total

    def column_sums(tiles, u):
        return jnp.concatenate([fold(tile * u) for tile in tiles], axis=1)

    def row_scale(rows, lanes):
        u = p_col[rows, :] / jnp.sum(lanes, axis=1, keepdims=True)
        u_ref[rows, :] = u
        return u

    def push_part(par, h):
        acc = jnp.zeros((8, part_w), jnp.float32)
        for k in range(n_blk):
            rows = pl.ds(k * BLK, BLK)
            acc = acc + column_sums(lane_tiles(kern, rows, part_cols(h)), u_ref[rows, :])
        push(par, h, jnp.sum(acc, axis=0, keepdims=True))

    def cost_tiles(rows):
        return [(a_col[rows, :] + b_row[:, j:j + LANES]) - 2.0 * cross[rows, j:j + LANES] for j in range(0, cross.shape[1], LANES)]

    def first_sweep(step):
        inv_eps = 1.0 / jnp.full((1, 1), eps_ref[step], jnp.float32)
        for k in range(n_blk):
            rows = pl.ds(k * BLK, BLK)
            tiles = cost_tiles(rows)
            low = tiles[0]
            for tile in tiles[1:]:
                low = jnp.minimum(low, tile)
            low = jnp.min(low, axis=1, keepdims=True)
            tiles = [jnp.exp((low - tile) * inv_eps) for tile in tiles]
            for j, tile in enumerate(tiles):
                kern[rows, j * LANES:(j + 1) * LANES] = tile
            row_scale(rows, row_sums(tiles))
        for h in range(n_part):
            push_part(0, h)

    def scale(par, h):
        return q_row[:, part_cols(h)] / pull(par, h)

    def sweep(i, carry):
        prev, cur = (i + 1) % 2, i % 2

        def weighted(h, v):
            def sums(rows):
                tiles = lane_tiles(kern, rows, part_cols(h))
                return row_sums([tile * v[:, j * LANES:(j + 1) * LANES] for j, tile in enumerate(tiles)])
            return sums

        for h in range(n_part - 1):
            sums = weighted(h, scale(prev, h))
            for k in range(n_blk):
                rows = pl.ds(k * BLK, BLK)
                row_sum[rows, :] = sums(rows) if h == 0 else row_sum[rows, :] + sums(rows)
        sums = weighted(n_part - 1, scale(prev, n_part - 1))
        acc = jnp.zeros((8, part_w), jnp.float32)
        for k in range(n_blk):
            rows = pl.ds(k * BLK, BLK)
            lanes = sums(rows) if n_part == 1 else row_sum[rows, :] + sums(rows)
            acc = acc + column_sums(lane_tiles(kern, rows, part_cols(0)), row_scale(rows, lanes))
        push(cur, 0, jnp.sum(acc, axis=0, keepdims=True))
        for h in range(1, n_part):
            push_part(cur, h)
        return carry

    v_ref = loss_ref

    def outer(step, carry):
        first_sweep(step)
        lax.fori_loop(1, SWEEPS, sweep, 0)
        for h in range(n_part):
            v_ref[:, part_cols(h)] = scale((SWEEPS - 1) % 2, h)
        for c in range(n_chunk):
            cols = pl.ds(pl.multiple_of(me_c * width + c * LANES, LANES), LANES)
            for k in range(n_blk):
                rows = pl.ds(k * BLK, BLK)
                plan = u_ref[rows, :] * kern[rows, cols] * v_ref[:, cols]
                t_ref[rows, c * LANES:(c + 1) * LANES] = plan
                tp[me_r, c, rows, :] = plan.astype(jnp.bfloat16)
            if c == 0:
                t_start(0)
        cost((step + 1) % 2)
        return carry

    prologue()
    lax.fori_loop(0, n_steps, outer, 0)

    acc = jnp.zeros((8, cross.shape[1]), jnp.float32)
    for k in range(n_blk):
        rows = pl.ds(k * BLK, BLK)
        plan = [u_ref[rows, :] * kern[rows, j:j + LANES] * v_ref[:, j:j + LANES] for j in range(0, cross.shape[1], LANES)]
        acc = acc + jnp.concatenate([fold(x * y) for x, y in zip(cost_tiles(rows), plan)], axis=1)
    total = jnp.sum(acc, axis=0, keepdims=True)
    half_sum = total[:, part_cols(0)]
    for h in range(1, n_part):
        half_sum = half_sum + total[:, part_cols(h)]
    push(SWEEPS % 2, 0, half_sum)
    loss_ref[...] = jnp.broadcast_to(jnp.sum(pull(SWEEPS % 2, 0), axis=1, keepdims=True), loss_ref.shape)


def solution(mesh):
    grid_spec = P(("pairs", "rows"), "cols")
    n_rows, n_cols = mesh.shape["rows"], mesh.shape["cols"]

    def local_fn(c1_blk, c2_blk, t0_blk, p_blk, q_blk, eps_blk):
        height, width = t0_blk.shape
        full = width * n_cols
        n_chunk = width // LANES
        n_piece = c1_blk.shape[1] // PIECE
        n_steps = eps_blk.shape[0]
        vmem = pl.BlockSpec(memory_space=pltpu.VMEM)
        f32, b16, dma = jnp.float32, jnp.bfloat16, pltpu.SemaphoreType.DMA
        plan, loss = pl.pallas_call(
            functools.partial(gw_kernel, n_rows, n_cols, n_steps, N_PART),
            out_shape=(jax.ShapeDtypeStruct((height, width), f32), jax.ShapeDtypeStruct((1, full), f32)),
            in_specs=[pl.BlockSpec(memory_space=pltpu.SMEM), pl.BlockSpec(memory_space=pl.ANY)] + [vmem] * 4,
            out_specs=(vmem, vmem),
            scratch_shapes=[
                pltpu.VMEM((n_cols * n_piece, height, PIECE), b16),
                pltpu.VMEM((n_rows, n_chunk, height, LANES), b16),
                pltpu.VMEM((2, n_cols, n_chunk, height, LANES), b16),
                pltpu.VMEM((n_chunk, height, LANES), f32),
                pltpu.VMEM((height, full), f32),
                pltpu.VMEM((height, full), f32),
                pltpu.VMEM((height, LANES), f32),
                pltpu.VMEM((height, LANES), f32),
                pltpu.VMEM((2, N_PART, n_rows, 1, full // N_PART), f32),
                pltpu.VMEM((2, height, PIECE), f32),
                pltpu.VMEM((height, LANES), f32),
                pltpu.VMEM((height, LANES), f32),
                pltpu.VMEM((height, LANES), f32),
                pltpu.VMEM((1, full), f32),
                pltpu.VMEM((1, full), f32),
                pltpu.VMEM((n_rows, n_cols) + c2_blk.shape, b16),
                pltpu.VMEM((full, full), b16),
                pltpu.VMEM((n_rows, 1, height), f32),
                pltpu.VMEM((n_cols, 1, width), f32),
                pltpu.VMEM((n_cols, 1, width), f32),
                pltpu.VMEM((n_rows, 1, width), f32),
                pltpu.VMEM((n_cols, 1, height), f32),
                dma((n_chunk, 14)), dma((n_rows, n_chunk, 2)),
                dma((n_chunk, 6)), dma((2, n_cols, n_chunk, 2)),
                dma((2, N_PART)), dma((2, N_PART)),
                dma((3 * n_piece,)), dma((n_cols * n_piece,)),
                dma((7, n_rows)), dma((7, n_rows)), dma((2,)),
            ],
            compiler_params=pltpu.CompilerParams(collective_id=0, has_side_effects=True, vmem_limit_bytes=62 * 2**20),
        )(eps_blk, c1_blk, c2_blk, t0_blk, p_blk[None, :], q_blk[None, :])
        return plan, loss[0, :1]

    return jax.shard_map(local_fn, mesh=mesh, in_specs=(grid_spec, grid_spec, grid_spec, P(("pairs", "rows")), P(("pairs", "cols")), P("pairs")), out_specs=(grid_spec, P("pairs")), check_vma=False)
```

```python
import functools

import jax
import jax.numpy as jnp
from jax import lax
from jax.experimental import pallas as pl
from jax.experimental.pallas import tpu as pltpu
from jax.sharding import PartitionSpec as P

SWEEPS = 10
MESH = pl.DeviceIdType.MESH
BLK = 128
LANES = 128
PIECE = 256
N_PART = 1


def gw_kernel(n_rows, n_cols, n_steps, n_part, eps_ref, c1_ref, c2_ref, t0_ref, p_ref, q_ref,
              t_ref, loss_ref, c1s, tp, ap, lead, cross, kern, u_ref, row_sum, red,
              stage, a_acc, a_col, p_col, b_row, q_row, c2f, c2s, p_all, q_all, b_all, b_red, a_red,
              t_send, t_recv, a_send, a_recv, s_send, s_recv, c_send, c_recv, x_send, x_recv, ld_sem):
    me_r = lax.axis_index("rows")
    me_c = lax.axis_index("cols")
    chip, core = me_r // 2, me_r % 2
    n_chips = n_rows // 2
    height, width = t0_ref.shape
    half = height // 2
    n_chunk = width // LANES
    n_piece = c1_ref.shape[1] // PIECE
    per_slot = height // PIECE
    n_blk = height // BLK

    def row_id(chip_off, core_sel):
        return ((chip + chip_off + n_chips) % n_chips) * 2 + core_sel

    sib = row_id(0, 1 - core)
    right, left, far = row_id(1, core), row_id(-1, core), row_id(2, core)
    up, down, opp = (me_c + 1) % n_cols, (me_c + n_cols - 1) % n_cols, (me_c + 2) % n_cols

    first_load = pltpu.make_async_copy(c1_ref.at[:, pl.ds(0, PIECE)], stage.at[0], ld_sem.at[0])
    first_load.start()
    barrier = pltpu.get_barrier_semaphore()
    for d in range(1, n_rows):
        pl.semaphore_signal(barrier, inc=1, device_id={"rows": (me_r + d) % n_rows}, device_id_type=MESH)
    for d in range(1, n_cols):
        pl.semaphore_signal(barrier, inc=1, device_id={"cols": (me_c + d) % n_cols}, device_id_type=MESH)
    pl.semaphore_wait(barrier, n_rows + n_cols - 2)

    def share(idx, axis, ref_of):
        me, n = (me_r, n_rows) if axis == "rows" else (me_c, n_cols)

        def copy(slot, d):
            return pltpu.make_async_remote_copy(src_ref=ref_of(slot), dst_ref=ref_of(slot), send_sem=x_send.at[idx, d],
                                                recv_sem=x_recv.at[idx, slot], device_id={axis: (me + d) % n}, device_id_type=MESH)

        for d in range(1, n):
            copy(me, d).start()

        def finish():
            for d in range(1, n):
                copy((me + d) % n, d).wait_recv()
            for d in range(1, n):
                copy(me, d).wait_send()

        return finish

    part_w = kern.shape[1] // n_part

    peers = [far, row_id(2, 1 - core), left, right, row_id(-1, 1 - core), row_id(1, 1 - core), sib]

    def sum_copy(par, h, ref, target):
        return pltpu.make_async_remote_copy(src_ref=ref, dst_ref=ref, send_sem=s_send.at[par, h], recv_sem=s_recv.at[par, h],
                                            device_id={"rows": target}, device_id_type=MESH)

    def push(par, h, value):
        red[par, h, me_r] = value
        for target in peers:
            sum_copy(par, h, red.at[par, h, me_r], target).start()

    def pull(par, h):
        every = sum_copy(par, h, red.at[par, h, pl.ds(0, n_rows - 1)], sib)
        every.wait_recv()
        total = red[par, h, 0]
        for d in range(1, n_rows):
            total = total + red[par, h, d]
        every.wait_send()
        return total

    def t_copy(slot, chunk, part, target, send_idx):
        ref = tp.at[slot, chunk, pl.ds(part * half, half)]
        return pltpu.make_async_remote_copy(src_ref=ref, dst_ref=ref, send_sem=t_send.at[chunk, send_idx],
                                            recv_sem=t_recv.at[slot, chunk, part], device_id={"rows": target}, device_id_type=MESH)

    t_sent = []

    def t_push(slot, chunk, part, target, send_idx):
        copy = t_copy(slot, chunk, part, target, send_idx)
        copy.start()
        t_sent.append(copy)

    def t_take(slot, chunk, part):
        t_copy(slot, chunk, part, sib, 0).wait_recv()

    def t_start(chunk):
        for part in (0, 1):
            t_push(me_r, chunk, part, right, part)
            t_push(me_r, chunk, 1 - part, left, 2 + part)
        for part in (0, 1):
            t_push(me_r, chunk, part, sib, 4 + part)

    def t_near(chunk):
        t_take(left, chunk, 0)
        t_push(left, chunk, 0, right, 6)
        t_take(right, chunk, 1)
        t_push(right, chunk, 1, left, 7)
        t_push(left, chunk, 0, sib, 8)
        t_push(right, chunk, 1, sib, 9)

    def t_rest(chunk):
        t_take(left, chunk, 1)
        t_push(left, chunk, 1, sib, 10)
        t_take(right, chunk, 0)
        t_push(right, chunk, 0, sib, 11)

    def t_far(chunk):
        for part in (0, 1):
            t_take(far, chunk, part)
            t_push(far, chunk, part, sib, 12 + part)

    def t_sib(chunk, chip_off):
        slot = row_id(chip_off, 1 - core)
        t_take(slot, chunk, 0)
        t_take(slot, chunk, 1)
        return slot

    def t_done():
        for copy in t_sent:
            copy.wait_send()
        t_sent.clear()

    def a_copy(par, slot, chunk, part, target, send_idx):
        ref = ap.at[par, slot, chunk, pl.ds(part * half, half)]
        return pltpu.make_async_remote_copy(src_ref=ref, dst_ref=ref, send_sem=a_send.at[chunk, send_idx],
                                            recv_sem=a_recv.at[par, slot, chunk, part], device_id={"cols": target}, device_id_type=MESH)

    a_sent = []

    def a_push(par, slot, chunk, part, target, send_idx):
        copy = a_copy(par, slot, chunk, part, target, send_idx)
        copy.start()
        a_sent.append(copy)

    def a_take(par, slot, chunk, part):
        a_copy(par, slot, chunk, part, up, 0).wait_recv()

    def a_start(par, chunk):
        ap[par, me_c, chunk] = lead[chunk].astype(jnp.bfloat16)
        for part in (0, 1):
            a_push(par, me_c, chunk, part, up, part)
            a_push(par, me_c, chunk, 1 - part, down, 2 + part)

    def a_near(par, chunk):
        a_take(par, down, chunk, 0)
        a_push(par, down, chunk, 0, up, 4)
        a_take(par, up, chunk, 1)
        a_push(par, up, chunk, 1, down, 5)

    def a_rest(par, chunk):
        a_take(par, down, chunk, 1)
        a_take(par, up, chunk, 0)

    def a_far(par, chunk):
        a_take(par, opp, chunk, 0)
        a_take(par, opp, chunk, 1)

    def a_done():
        for copy in a_sent:
            copy.wait_send()
        a_sent.clear()

    def c1_slot(slot):
        return jnp.concatenate([c1s[slot * per_slot + j] for j in range(per_slot)], axis=1)

    def lead_add(slot, chunk, part=None, first=False):
        if part is None:
            prod = jnp.dot(c1_slot(slot), tp[slot, chunk], preferred_element_type=jnp.float32)
        else:
            hop = per_slot // 2
            block = jnp.concatenate([c1s[slot * per_slot + part * hop + j] for j in range(hop)], axis=1)
            prod = jnp.dot(block, tp[slot, chunk, part * half:(part + 1) * half], preferred_element_type=jnp.float32)
        lead[chunk] = prod if first else lead[chunk] + prod

    def lead_both(slot):
        plan = jnp.concatenate([tp[slot, k] for k in range(n_chunk)], axis=1)
        prod = jnp.dot(c1_slot(slot), plan, preferred_element_type=jnp.float32)
        for k in range(n_chunk):
            lead[k] = lead[k] + prod[:, k * LANES:(k + 1) * LANES]

    def cross_add(par, pairs, first=False):
        block = jnp.concatenate([ap[par, slot, k] for slot, k in pairs], axis=1)
        rows = [pl.ds(pl.multiple_of(slot * width + k * LANES, LANES), LANES) for slot, k in pairs]
        right_side = jnp.concatenate([c2s[r, :] for r in rows], axis=0)
        prod = jnp.dot(block, right_side, preferred_element_type=jnp.float32)
        cross[...] = prod if first else cross[...] + prod

    def whole(slot):
        return [(slot, k) for k in range(n_chunk)]

    def piece_load(i):
        cols = pl.ds(pl.multiple_of(i * PIECE, PIECE), PIECE)
        return pltpu.make_async_copy(c1_ref.at[:, cols], stage.at[i % 2], ld_sem.at[i % 2])

    def piece_copy(piece, target, send_idx):
        return pltpu.make_async_remote_copy(src_ref=c1s.at[piece], dst_ref=c1s.at[piece], send_sem=c_send.at[send_idx],
                                            recv_sem=c_recv.at[piece], device_id={"cols": target}, device_id_type=MESH)

    def prologue():
        def piece_send(i):
            piece = me_c * n_piece + i
            c1s[piece] = stage[i % 2].astype(jnp.bfloat16)
            piece_copy(piece, up, i).start()
            piece_copy(piece, down, n_piece + i).start()

        def piece_sum(i):
            block = stage[i % 2]
            where = (me_c * n_piece + i) * PIECE
            p_row = p_all[where // height, :, pl.ds(pl.multiple_of(where % height, PIECE), PIECE)]
            sq = block * block * p_row
            acc = a_acc[...]
            for k in range(PIECE // LANES):
                acc = acc + sq[:, k * LANES:(k + 1) * LANES]
            a_acc[...] = acc

        piece_load(0).wait()
        piece_load(1).start()
        piece_send(0)
        p_all[me_r] = p_ref[...]
        p_fin = share(0, "rows", lambda s: p_all.at[s])
        q_all[me_c] = q_ref[...]
        q_fin = share(1, "cols", lambda s: q_all.at[s])
        c2f[me_r, me_c] = c2_ref[...].astype(jnp.bfloat16)
        c2y_fin = share(2, "cols", lambda s: c2f.at[me_r, s])
        for k in range(n_chunk):
            tp[me_r, k] = t0_ref[:, k * LANES:(k + 1) * LANES].astype(jnp.bfloat16)
        for k in range(n_chunk):
            t_start(k)
        a_acc[...] = jnp.zeros_like(a_acc)
        p_fin()
        piece_sum(0)

        def own_piece(i, carry):
            piece_load(i).wait()

            @pl.when(i + 1 < n_piece)
            def _():
                piece_load(i + 1).start()

            piece_send(i)
            piece_sum(i)
            return carry

        lax.fori_loop(1, n_piece, own_piece, 0)
        q_fin()
        q_row[...] = jnp.concatenate([q_all[k] for k in range(n_cols)], axis=1)
        a_red[me_c] = jnp.sum(a_acc[...].T, axis=0, keepdims=True)
        a_fin = share(3, "cols", lambda s: a_red.at[s])
        low = me_r * c2_ref.shape[0]
        q_piece = q_all[low // width, :, pl.ds(pl.multiple_of(low % width, LANES), LANES)]
        q_col = jnp.broadcast_to(q_piece, (LANES, LANES)).T
        sq = c2_ref[...] * c2_ref[...]
        b_red[me_r] = jnp.sum(sq * q_col[:, :1], axis=0, keepdims=True)
        b_fin = share(4, "rows", lambda s: b_red.at[s])
        p_col[...] = jnp.broadcast_to(p_ref[...], (LANES, height)).T
        c2y_fin()
        c2x_fin = share(5, "rows", lambda s: c2f.at[s])
        for k in range(n_chunk):
            t_near(k)
        for k in range(n_chunk):
            t_rest(k)
        b_fin()
        total = b_red[0]
        for s in range(1, n_rows):
            total = total + b_red[s]
        b_all[me_c] = total
        ball_fin = share(6, "cols", lambda s: b_all.at[s])
        for k in range(n_chunk):
            t_far(k)
        for k in range(n_chunk):
            for off in (0, -1, 1, 2):
                t_sib(k, off)
        t_done()
        lead[...] = jnp.zeros_like(lead)

        def group(which):
            def body(j, carry):
                lead_both(which * (n_piece // per_slot) + j)
                return carry

            lax.fori_loop(0, n_piece // per_slot, body, 0)

        group(me_c)
        hop = n_piece // 2
        for i in range(n_piece):
            piece_copy(down * n_piece + i, up, 0).wait_recv()
            if i < hop:
                piece_copy(down * n_piece + i, up, 2 * n_piece + i).start()
            piece_copy(up * n_piece + i, up, 0).wait_recv()
            if i >= hop:
                piece_copy(up * n_piece + i, down, 2 * n_piece + i).start()
        group(down)
        group(up)
        a_fin()
        total = a_red[0]
        for s in range(1, n_cols):
            total = total + a_red[s]
        a_col[...] = jnp.broadcast_to(total, (LANES, height)).T
        ball_fin()
        b_row[...] = jnp.concatenate([b_all[k] for k in range(n_cols)], axis=1)
        c2x_fin()
        depth = c2_ref.shape[0]
        for r in range(n_rows):
            for c in range(n_cols):
                c2s[r * depth:(r + 1) * depth, c * width:(c + 1) * width] = c2f[r, c] * 2
        for i in range(n_piece):
            piece_copy(opp * n_piece + i, up, 0).wait_recv()
        group(opp)
        for i in range(n_piece):
            piece_copy(me_c * n_piece + i, up, i).wait_send()
            piece_copy(me_c * n_piece + i, down, n_piece + i).wait_send()
            if i < hop:
                piece_copy(down * n_piece + i, up, 2 * n_piece + i).wait_send()
            else:
                piece_copy(up * n_piece + i, down, 2 * n_piece + i).wait_send()

        for k in range(n_chunk):
            a_start(0, k)
        cross_add(0, whole(me_c), True)
        for k in range(n_chunk):
            a_near(0, k)
        for k in range(n_chunk):
            a_rest(0, k)
        cross_add(0, whole(down))
        cross_add(0, whole(up))
        for k in range(n_chunk):
            a_far(0, k)
        cross_add(0, [(opp, k) for k in range(n_chunk - 1)])
        a_done()

    def t_sib_part(chunk, chip_off, part):
        slot = row_id(chip_off, 1 - core)
        t_take(slot, chunk, part)
        lead_add(slot, chunk, part)

    def cost(par):
        def near(chunk):
            lead_add(left, chunk, 0)
            lead_add(right, chunk, 1)
            t_sib_part(chunk, -1, 0)
            t_sib_part(chunk, 1, 1)

        def rest(chunk):
            t_rest(chunk)
            lead_add(left, chunk, 1)
            lead_add(right, chunk, 0)
            t_sib_part(chunk, -1, 1)
            t_sib_part(chunk, 1, 0)

        def late(chunk):
            t_far(chunk)
            lead_add(far, chunk)
            lead_add(t_sib(chunk, 2), chunk)
            a_start(par, chunk)

        lead_add(me_r, 0, None, True)
        lead_add(t_sib(0, 0), 0)
        t_near(0)
        t_start(1)
        near(0)
        lead_add(me_r, 1, None, True)
        lead_add(t_sib(1, 0), 1)
        rest(0)
        late(0)
        t_near(1)
        near(1)
        rest(1)
        a_near(par, 0)
        late(1)
        a_rest(par, 0)
        cross_add(par, whole(me_c), True)
        cross_add(par, [(down, 0), (up, 0)])
        a_far(par, 0)
        cross_add(par, [(opp, 0)])
        a_near(par, 1)
        a_rest(par, 1)
        cross_add(par, [(down, 1), (up, 1)])
        a_far(par, 1)
        t_done()
        a_done()

    def fold(block):
        return jnp.sum(block.reshape(BLK // 8, 8, block.shape[1]), axis=0)

    def part_cols(h):
        return slice(h * part_w, (h + 1) * part_w)

    def lane_tiles(ref, rows, cols):
        return [ref[rows, j:j + LANES] for j in range(cols.start, cols.stop, LANES)]

    def row_sums(tiles):
        total = tiles[0]
        for tile in tiles[1:]:
            total = total + tile
        return total

    def column_sums(tiles, u):
        return jnp.concatenate([fold(tile * u) for tile in tiles], axis=1)

    def row_scale(rows, lanes):
        u = p_col[rows, :] / jnp.sum(lanes, axis=1, keepdims=True)
        u_ref[rows, :] = u
        return u

    def push_part(par, h):
        acc = jnp.zeros((8, part_w), jnp.float32)
        for k in range(n_blk):
            rows = pl.ds(k * BLK, BLK)
            acc = acc + column_sums(lane_tiles(kern, rows, part_cols(h)), u_ref[rows, :])
        push(par, h, jnp.sum(acc, axis=0, keepdims=True))

    def cost_tiles(k, par):
        rows = pl.ds(k * BLK, BLK)
        last = pl.ds(pl.multiple_of(opp * width + (n_chunk - 1) * LANES, LANES), LANES)
        twice = cross[rows, :] + jnp.dot(ap[par, opp, n_chunk - 1, rows, :], c2s[last, :], preferred_element_type=jnp.float32)
        return [(a_col[rows, :] + b_row[:, j:j + LANES]) - twice[:, j:j + LANES] for j in range(0, cross.shape[1], LANES)]

    def first_sweep(step):
        inv_eps = 1.0 / jnp.full((1, 1), eps_ref[step], jnp.float32)
        for k in range(n_blk):
            rows = pl.ds(k * BLK, BLK)
            tiles = cost_tiles(k, step % 2)
            low = tiles[0]
            for tile in tiles[1:]:
                low = jnp.minimum(low, tile)
            low = jnp.min(low, axis=1, keepdims=True)
            tiles = [jnp.exp((low - tile) * inv_eps) for tile in tiles]
            for j, tile in enumerate(tiles):
                kern[rows, j * LANES:(j + 1) * LANES] = tile
            row_scale(rows, row_sums(tiles))
        for h in range(n_part):
            push_part(0, h)

    def scale(par, h):
        return q_row[:, part_cols(h)] / pull(par, h)

    def sweep(i, carry):
        prev, cur = (i + 1) % 2, i % 2

        def weighted(h, v):
            def sums(rows):
                tiles = lane_tiles(kern, rows, part_cols(h))
                return row_sums([tile * v[:, j * LANES:(j + 1) * LANES] for j, tile in enumerate(tiles)])
            return sums

        for h in range(n_part - 1):
            sums = weighted(h, scale(prev, h))
            for k in range(n_blk):
                rows = pl.ds(k * BLK, BLK)
                row_sum[rows, :] = sums(rows) if h == 0 else row_sum[rows, :] + sums(rows)
        sums = weighted(n_part - 1, scale(prev, n_part - 1))
        acc = jnp.zeros((8, part_w), jnp.float32)
        for k in range(n_blk):
            rows = pl.ds(k * BLK, BLK)
            lanes = sums(rows) if n_part == 1 else row_sum[rows, :] + sums(rows)
            acc = acc + column_sums(lane_tiles(kern, rows, part_cols(0)), row_scale(rows, lanes))
        push(cur, 0, jnp.sum(acc, axis=0, keepdims=True))
        for h in range(1, n_part):
            push_part(cur, h)
        return carry

    v_ref = loss_ref

    def outer(step, carry):
        first_sweep(step)
        lax.fori_loop(1, SWEEPS, sweep, 0)
        for h in range(n_part):
            v_ref[:, part_cols(h)] = scale((SWEEPS - 1) % 2, h)
        for c in range(n_chunk):
            cols = pl.ds(pl.multiple_of(me_c * width + c * LANES, LANES), LANES)
            for k in range(n_blk):
                rows = pl.ds(k * BLK, BLK)
                plan = u_ref[rows, :] * kern[rows, cols] * v_ref[:, cols]
                t_ref[rows, c * LANES:(c + 1) * LANES] = plan
                tp[me_r, c, rows, :] = plan.astype(jnp.bfloat16)
            if c == 0:
                t_start(0)
        cost((step + 1) % 2)
        return carry

    prologue()
    lax.fori_loop(0, n_steps, outer, 0)

    acc = jnp.zeros((8, cross.shape[1]), jnp.float32)
    for k in range(n_blk):
        rows = pl.ds(k * BLK, BLK)
        plan = [u_ref[rows, :] * kern[rows, j:j + LANES] * v_ref[:, j:j + LANES] for j in range(0, cross.shape[1], LANES)]
        acc = acc + jnp.concatenate([fold(x * y) for x, y in zip(cost_tiles(k, n_steps % 2), plan)], axis=1)
    total = jnp.sum(acc, axis=0, keepdims=True)
    half_sum = total[:, part_cols(0)]
    for h in range(1, n_part):
        half_sum = half_sum + total[:, part_cols(h)]
    push(SWEEPS % 2, 0, half_sum)
    loss_ref[...] = jnp.broadcast_to(jnp.sum(pull(SWEEPS % 2, 0), axis=1, keepdims=True), loss_ref.shape)


def solution(mesh):
    grid_spec = P(("pairs", "rows"), "cols")
    n_rows, n_cols = mesh.shape["rows"], mesh.shape["cols"]

    def local_fn(c1_blk, c2_blk, t0_blk, p_blk, q_blk, eps_blk):
        height, width = t0_blk.shape
        full = width * n_cols
        n_chunk = width // LANES
        n_piece = c1_blk.shape[1] // PIECE
        n_steps = eps_blk.shape[0]
        vmem = pl.BlockSpec(memory_space=pltpu.VMEM)
        f32, b16, dma = jnp.float32, jnp.bfloat16, pltpu.SemaphoreType.DMA
        plan, loss = pl.pallas_call(
            functools.partial(gw_kernel, n_rows, n_cols, n_steps, N_PART),
            out_shape=(jax.ShapeDtypeStruct((height, width), f32), jax.ShapeDtypeStruct((1, full), f32)),
            in_specs=[pl.BlockSpec(memory_space=pltpu.SMEM), pl.BlockSpec(memory_space=pl.ANY)] + [vmem] * 4,
            out_specs=(vmem, vmem),
            scratch_shapes=[
                pltpu.VMEM((n_cols * n_piece, height, PIECE), b16),
                pltpu.VMEM((n_rows, n_chunk, height, LANES), b16),
                pltpu.VMEM((2, n_cols, n_chunk, height, LANES), b16),
                pltpu.VMEM((n_chunk, height, LANES), f32),
                pltpu.VMEM((height, full), f32),
                pltpu.VMEM((height, full), f32),
                pltpu.VMEM((height, LANES), f32),
                pltpu.VMEM((height, LANES), f32),
                pltpu.VMEM((2, N_PART, n_rows, 1, full // N_PART), f32),
                pltpu.VMEM((2, height, PIECE), f32),
                pltpu.VMEM((height, LANES), f32),
                pltpu.VMEM((height, LANES), f32),
                pltpu.VMEM((height, LANES), f32),
                pltpu.VMEM((1, full), f32),
                pltpu.VMEM((1, full), f32),
                pltpu.VMEM((n_rows, n_cols) + c2_blk.shape, b16),
                pltpu.VMEM((full, full), b16),
                pltpu.VMEM((n_rows, 1, height), f32),
                pltpu.VMEM((n_cols, 1, width), f32),
                pltpu.VMEM((n_cols, 1, width), f32),
                pltpu.VMEM((n_rows, 1, width), f32),
                pltpu.VMEM((n_cols, 1, height), f32),
                dma((n_chunk, 14)), dma((n_rows, n_chunk, 2)),
                dma((n_chunk, 6)), dma((2, n_cols, n_chunk, 2)),
                dma((2, N_PART)), dma((2, N_PART)),
                dma((3 * n_piece,)), dma((n_cols * n_piece,)),
                dma((7, n_rows)), dma((7, n_rows)), dma((2,)),
            ],
            compiler_params=pltpu.CompilerParams(collective_id=0, has_side_effects=True, vmem_limit_bytes=62 * 2**20),
        )(eps_blk, c1_blk, c2_blk, t0_blk, p_blk[None, :], q_blk[None, :])
        return plan, loss[0, :1]

    return jax.shard_map(local_fn, mesh=mesh, in_specs=(grid_spec, grid_spec, grid_spec, P(("pairs", "rows")), P(("pairs", "cols")), P("pairs")), out_specs=(grid_spec, P("pairs")), check_vma=False)
```
